256 devices in a mesh: row: 8 (over y, core), th: 8 (over z), ph: 4 (over x).
Axes of the slice: x: 4, y: 4, z: 8, core: 2. Of those that a mesh axis runs over, the one named last changes fastest.
Arguments:
- fields: float32 [6, 128, 128, 512], P(None, 'row', 'th', 'ph'), may hold values from -6 to 6
- lapse_field: float32 [128, 128, 512], P('row', 'th', 'ph'), may hold values from 0.3 to 1
- excision: int32 [128, 128, 512], P('row', 'th', 'ph'), may hold values 0 or 1
- sample_cells: int32 [128, 128, 4], P('row', 'th', 'ph'), may hold values from 0 to 127
- old_basis: float32 [252, 196608], P(None, ('row', 'th', 'ph'))
Outputs:
- new_fields: float32 [6, 128, 128, 512], P(None, 'row', 'th', 'ph')
- basis_out: float32 [256, 196608], P(None, ('row', 'th', 'ph'))
- factor: float32 [256, 256], replicated
The draws below stay inside these ranges and needn't reach their ends.
Inputs may be any that keep to these rules, and one draw needn't show every extreme that they name: `excision`: 1 marks an excised cell.
All inputs are finite; a program needn't handle non-finite values. No bound on the sum of `excision` on one device may be relied on, other than what follows from the above.
Results may differ from the reference program's by a relative error of at most 0.007.
Values sent between devices are 32-bit elements; how exact they have to be, the bound alone decides.
A program may use at most 64 MiB of HBM per device.

```python
import math
import jax
import jax.numpy as jnp
from jax import lax

CR = 16
CT = 16
CP = 128
SPACING = 128
OLD = 252
SROWS = 768
NR = 128
NT = 128
NP = 512
ROWS = 196608
N_ROW = 8
N_TH = 8
N_PH = 4


def draw_old_basis(key, part):
    keys = jax.random.split(jax.random.fold_in(key, 71), 5)
    normal_part = jax.random.normal(keys[0], (OLD, ROWS), jnp.float32)
    mixed = normal_part + 0.5 * jnp.roll(normal_part, 1, axis=0)
    column_scale = jnp.exp(jax.random.uniform(keys[1], (OLD, 1), jnp.float32, math.log(0.5), math.log(2.0)))
    row_factor = jnp.exp(jax.random.uniform(keys[2], (1, ROWS), jnp.float32, math.log(0.3), math.log(3.0)))
    block_count = ROWS // SROWS
    block_scale = jnp.exp(jax.random.uniform(keys[4], (block_count,), jnp.float32, 0.0, math.log(30.0)))
    block_rows = jnp.repeat(block_scale, SROWS, total_repeat_length=ROWS)[None, :]
    return mixed * column_scale * row_factor * block_rows


def place_ends(entries, rng, smallest, largest):
    place = [jax.random.randint(jax.random.fold_in(rng, axis), (), 0, length) for axis, length in enumerate(entries.shape)]
    main_axis = entries.shape.index(max(entries.shape))
    neighbour = place[:main_axis] + [(place[main_axis] + 1) % entries.shape[main_axis]] + place[main_axis + 1:]
    return entries.at[tuple(place)].set(smallest).at[tuple(neighbour)].set(largest)


def steps_of(own_key, extent, cuts, smallest, high):
    def one(dim, blocks):
        draws = jax.random.uniform(jax.random.fold_in(jax.random.fold_in(own_key, 6), dim), (blocks,), jnp.float32, smallest / len(cuts), high / len(cuts))
        return jnp.repeat(jnp.exp(draws), extent[dim] // blocks).reshape((-1,) + (1,) * (len(extent) - dim - 1))

    loudness = one(*cuts[0])
    for cut in cuts[1:]:
        loudness = loudness * one(*cut)
    return loudness


def centred(stream_key, shape, deviation, most, shards=(), kind=jnp.bfloat16):
    array = deviation * jax.random.normal(stream_key, shape, jnp.float32)
    if shards:
        array = array * steps_of(stream_key, shape, shards, -0.22, 0.18)
    return jnp.clip(array, -most, most).astype(kind)


def setup_inputs(seed: int = 0) -> dict:
    streams_of = jax.random.split(jax.random.key(seed), 6)
    fields = centred(streams_of[0], (6, NR, NT, NP), 1.0, 6.0, ((1, 8), (2, 8), (3, 4)), jnp.float32)
    lapse_field = jnp.clip(0.3 + 0.7 * jax.random.uniform(streams_of[1], (NR, NT, NP), jnp.float32) ** steps_of(streams_of[1], (NR, NT, NP), ((0, 8), (1, 8), (2, 4)), -0.2, 0.2), 0.3, 1.0)
    excision = place_ends((jax.random.randint(streams_of[2], (NR, NT, NP), 0, 8) < 1).astype(jnp.int32), jax.random.fold_in(streams_of[2], 1), 0, 1)
    sample_cells = place_ends(jax.random.randint(streams_of[3], (NR, NT, NP // SPACING), 0, SPACING), jax.random.fold_in(streams_of[3], 1), 0, SPACING - 1).astype(jnp.int32)
    old_basis = draw_old_basis(jax.random.fold_in(streams_of[5], 71), 0)
    return dict(fields=fields, lapse_field=lapse_field, excision=excision, sample_cells=sample_cells, old_basis=old_basis)


damping_rate = 3.0
time_step = 0.3
azimuth_gain = 5.0

def shifted(padded, axis_dim, offset):
    lengths = [padded.shape[0] - 4, padded.shape[1] - 4, padded.shape[2] - 4]
    starts = [2, 2, 2]
    starts[axis_dim] = 2 + offset
    return padded[starts[0]:starts[0] + lengths[0], starts[1]:starts[1] + lengths[1], starts[2]:starts[2] + lengths[2]]

def derivative(padded, axis_dim):
    near_diff = shifted(padded, axis_dim, 1) - shifted(padded, axis_dim, -1)
    far_diff = shifted(padded, axis_dim, 2) - shifted(padded, axis_dim, -2)
    spacing_gain = azimuth_gain if axis_dim == 2 else 1.0
    return (8.0 * near_diff - far_diff) * (spacing_gain / 12.0)

def curl_of(padded, start_comp):
    first_part = padded[start_comp]
    second_part = padded[start_comp + 1]
    third_part = padded[start_comp + 2]
    return jnp.stack([derivative(third_part, 1) - derivative(second_part, 2), derivative(first_part, 2) - derivative(third_part, 0), derivative(second_part, 0) - derivative(first_part, 1)])

def rates(padded, fields, damping):
    electric = curl_of(padded, 3) - damping_rate * damping * fields[:3]
    magnetic = -curl_of(padded, 0) - damping_rate * damping * fields[3:]
    return jnp.concatenate([electric, magnetic])

def wrap_pad(product):
    beside_all = jnp.concatenate([product[..., -2:], product, product[..., :2]], axis=-1)
    return jnp.pad(beside_all, ((0, 0), (2, 2), (2, 2), (0, 0)))

def as_rows(sampled):
    shaped = sampled.reshape(3, N_ROW, CR, N_TH, CT, N_PH, CP // SPACING)
    return jnp.transpose(shaped, (1, 3, 5, 0, 2, 4, 6)).reshape(-1)

def reference(fields, lapse_field, excision, sample_cells, old_basis):
    damping = excision.astype(jnp.float32)
    section_one = fields + time_step * rates(wrap_pad(lapse_field * fields), fields, damping)
    rate_two = rates(wrap_pad(lapse_field * section_one), section_one, damping)
    new_fields = 0.5 * (fields + section_one + time_step * rate_two)
    rad_index = jnp.arange(NR).astype(jnp.float32)
    pol_index = jnp.arange(NT).astype(jnp.float32)
    radius = 1.0 + 2.0 * (rad_index + 0.5) / NR
    polar = jnp.pi * (pol_index + 0.5) / NT
    weight = radius[:, None] * jnp.sqrt(jnp.sin(polar))[None, :]

    def sample(field_set):
        grouped = field_set.reshape(6, NR, NT, NP // SPACING, SPACING)
        picked = jnp.take_along_axis(grouped, sample_cells[None, :, :, :, None].astype(jnp.int32), axis=4)[..., 0]
        return picked * weight[None, :, :, None]
    snap_one = sample(section_one)
    snap_two = sample(new_fields)
    snapshot = jnp.stack([as_rows(snap_one[:3]), as_rows(snap_one[3:]), as_rows(snap_two[:3]), as_rows(snap_two[3:])])
    matrix = jnp.concatenate([old_basis, snapshot], axis=0)
    gram_sum = jnp.dot(matrix, matrix.T, precision=lax.Precision.HIGHEST)
    factor_low = lax.linalg.cholesky(gram_sum)
    solved = lax.linalg.triangular_solve(factor_low, matrix, left_side=True, lower=True)
    row_scale = math.sqrt(ROWS)
    return (new_fields, solved * row_scale, factor_low.T / row_scale)
```

```python
import functools
import math

import jax
import jax.numpy as jnp
from jax import lax
from jax.experimental import pallas as pl
from jax.experimental.pallas import tpu as pltpu
from jax.sharding import PartitionSpec as P

MESH = pl.DeviceIdType.MESH
HIGH = lax.Precision.HIGHEST
VMEM = pl.BlockSpec(memory_space=pltpu.VMEM)
ANY = pl.BlockSpec(memory_space=pl.ANY)

damping_rate = 3.0
time_step = 0.3
azimuth_gain = 5.0

SLOT = {0: 0, 3: 1, 2: 2, 5: 3, 1: 4, 4: 5}
EDGE = {0: 0, 3: 1, 1: 2, 4: 3}


def nt(a, b):
    return lax.dot_general(a, b, (((1,), (1,)), ((), ())), precision=HIGH, preferred_element_type=jnp.float32)


def nn(a, b):
    return lax.dot_general(a, b, (((1,), (0,)), ((), ())), precision=HIGH, preferred_element_type=jnp.float32)


def tn(a, b):
    return lax.dot_general(a, b, (((0,), (0,)), ((), ())), precision=HIGH, preferred_element_type=jnp.float32)


def diff(near_high, near_low, far_high, far_low, gain):
    return (8.0 * (near_high - near_low) - (far_high - far_low)) * (gain / 12.0)


def comm_kernel(
    sizes,
    fields_ref, lapse_ref, excision_ref, cells_ref, old_ref,
    new_ref, gram_ref, cross_ref, snap_ref,
    field, lapse, excision, cells, old, mat, section, fresh, weighted, masked,
    padded, polar_out, polar_in, edge_out, edge_in,
    gram, full, pair, plane, deep, cross_plane, cross_deep,
    load_sem, store_sem, halo_send, halo_recv, send_sem, recv_sem,
):
    n_row, n_th, n_ph = sizes
    n_y = n_row // 2
    row, th, ph = lax.axis_index("row"), lax.axis_index("th"), lax.axis_index("ph")
    core, y = lax.rem(row, 2), lax.div(row, 2)
    spot = y * n_ph + ph
    half = n_y * n_ph
    chunks = 2 * half
    owner = core * half + spot
    cr, ct, cp = 16, 16, 128

    loads = [
        pltpu.make_async_copy(source, target, load_sem.at[k])
        for k, (source, target) in enumerate(
            ((old_ref, old), (fields_ref, field), (lapse_ref, lapse), (excision_ref, excision), (cells_ref, cells))
        )
    ]
    for load in loads:
        load.start()

    def place(index):
        which, rest = lax.div(index, half), lax.rem(index, half)
        return {"row": lax.div(rest, n_ph) * 2 + which, "ph": lax.rem(rest, n_ph)}

    def in_plane(d):
        return place(lax.rem(owner + d, chunks))

    def in_half(d):
        return place(core * half + lax.rem(spot + d, half))

    def along(d):
        return {"th": lax.rem(th + d, n_th)}

    barrier = pltpu.get_barrier_semaphore()
    for d in range(1, chunks):
        pl.semaphore_signal(barrier, inc=1, device_id=in_plane(d), device_id_type=MESH)
    for d in range(1, n_th):
        pl.semaphore_signal(barrier, inc=1, device_id=along(d), device_id_type=MESH)

    def send(source, target, device, k):
        copy = pltpu.make_async_remote_copy(
            src_ref=source, dst_ref=target, send_sem=send_sem.at[k], recv_sem=recv_sem.at[k],
            device_id=device, device_id_type=MESH,
        )
        copy.start()

    def landed(ref, k):
        pltpu.make_async_copy(ref, ref, recv_sem.at[k]).wait()

    def left(ref, k):
        pltpu.make_async_copy(ref, ref, send_sem.at[k]).wait()

    lane = lax.broadcasted_iota(jnp.int32, (ct, cp), 1)
    lane_pair = lax.shift_right_logical(lane, 1)

    loads[0].wait()
    mat[0:248] = old[0:248]
    mat[248:252] = old[248:252]
    mat[252:256] = jnp.zeros((4, mat.shape[1]), jnp.float32)
    product = nt(mat[...], mat[...])
    gram[...] = product.reshape(gram.shape)

    def keep_product(stage, c, i, value, edges):
        slot = SLOT[c]
        padded[stage, slot, i + 2, 8:24, :] = value
        if slot < 4:
            for s in range(2):
                polar_out[stage, 0, slot, s, pl.ds(i, 1), :] = value[s : s + 1]
                polar_out[stage, 1, slot, s, pl.ds(i, 1), :] = value[14 + s : 15 + s]
        if c in EDGE:
            t = EDGE[c] * cr + i
            here = lane_pair == t
            edges = (
                jnp.where(here, pltpu.roll(value, 2 * t, 1), edges[0]),
                jnp.where(here, pltpu.roll(value, lax.rem(2 * t + 2, cp), 1), edges[1]),
            )
        return edges

    def no_edges():
        return jnp.zeros((ct, cp), jnp.float32), jnp.zeros((ct, cp), jnp.float32)

    def first_products(i, edges):
        scale = lapse[i]
        for c in range(6):
            edges = keep_product(0, c, i, scale * field[c, i], edges)
        return edges

    def halo_copies(stage):
        rows = ((padded.at[stage, 2:6, 2:4, 8:24, :], padded.at[stage, 2:6, 18:20, 8:24, :], {"row": lax.rem(row + n_row - 1, n_row)}),
                (padded.at[stage, 2:6, 16:18, 8:24, :], padded.at[stage, 2:6, 0:2, 8:24, :], {"row": lax.rem(row + 1, n_row)}))
        polars = ((polar_out.at[stage, 0], polar_in.at[stage, 1], {"th": lax.rem(th + n_th - 1, n_th)}),
                  (polar_out.at[stage, 1], polar_in.at[stage, 0], {"th": lax.rem(th + 1, n_th)}))
        edges = ((edge_out.at[stage, 0], edge_in.at[stage, 1], {"ph": lax.rem(ph + n_ph - 1, n_ph)}),
                 (edge_out.at[stage, 1], edge_in.at[stage, 0], {"ph": lax.rem(ph + 1, n_ph)}))
        return [
            pltpu.make_async_remote_copy(
                src_ref=source, dst_ref=target, send_sem=halo_send.at[stage, k], recv_sem=halo_recv.at[stage, k],
                device_id=device, device_id_type=MESH,
            )
            for k, (source, target, device) in enumerate(rows + polars + edges)
        ]

    def keep_edges(stage, edges):
        edge_out[stage, 0] = edges[0]
        edge_out[stage, 1] = edges[1]

    for load in loads[1:]:
        load.wait()
    keep_edges(0, lax.fori_loop(0, cr, first_products, no_edges()))

    pl.semaphore_wait(barrier, chunks - 1 + n_th - 1)

    halos = [halo_copies(0), halo_copies(1)]
    for copy in halos[0]:
        copy.start()
    other = 1 - core
    send(gram.at[pl.ds(other * half, half)], pair, {"row": y * 2 + other}, 0)

    pol_index = (th * ct + lax.broadcasted_iota(jnp.int32, (ct, cp), 0)).astype(jnp.float32)
    polar = jnp.pi * (pol_index + 0.5) / (n_th * ct)
    polar_weight = jnp.sqrt(jnp.sin(polar))
    chosen = cells[...].T
    for i in range(cr):
        radius = 1.0 + 2.0 * ((row * cr + i).astype(jnp.float32) + 0.5) / (n_row * cr)
        weighted[i] = jnp.where(lane == chosen[:, i : i + 1], polar_weight * radius, 0.0)

    def rates(stage, i, c_values):
        damped = damping_rate * excision[i].astype(jnp.float32)
        lo_edge, hi_edge = edge_in[stage, 0], edge_in[stage, 1]
        for slot in range(4):
            for s in range(2):
                low = polar_in[stage, 0, slot, s, pl.ds(i, 1), :]
                high = polar_in[stage, 1, slot, s, pl.ds(i, 1), :]
                padded[stage, slot, i + 2, 6 + s : 7 + s, :] = jnp.where(th > 0, low, 0.0)
                padded[stage, slot, i + 2, 24 + s : 25 + s, :] = jnp.where(th < n_th - 1, high, 0.0)

        def rad(c):
            get = lambda o: padded[stage, SLOT[c], i + 2 + o, 8:24, :]
            return diff(get(1), get(-1), get(2), get(-2), 1.0)

        def pol(c):
            get = lambda o: padded[stage, SLOT[c], i + 2, 8 + o : 24 + o, :]
            return diff(get(1), get(-1), get(2), get(-2), 1.0)

        def azi(c):
            here = padded[stage, SLOT[c], i + 2, 8:24, :]
            t = EDGE[c] * cr + i
            low = pltpu.roll(lo_edge, cp - 2 - 2 * t, 1)
            high = pltpu.roll(hi_edge, lax.rem(cp - 2 * t, cp), 1)
            far_low = pltpu.roll(jnp.where(lane >= cp - 2, low, here), 2, 1)
            near_low = pltpu.roll(jnp.where(lane >= cp - 1, low, here), 1, 1)
            near_high = pltpu.roll(jnp.where(lane < 1, high, here), cp - 1, 1)
            far_high = pltpu.roll(jnp.where(lane < 2, high, here), cp - 2, 1)
            return diff(near_high, near_low, far_high, far_low, azimuth_gain)

        out = []
        for start, sign in ((3, 1.0), (0, -1.0)):
            curls = (pol(start + 2) - azi(start + 1), azi(start) - rad(start + 2), rad(start + 1) - pol(start))
            for k in range(3):
                c = len(out)
                out.append((curls[k] if sign > 0 else -curls[k]) - damped * c_values[c])
        return out

    def zero_ends(stage):
        low = padded[stage, 2:6, 0:2, 8:24, :]
        padded[stage, 2:6, 0:2, 8:24, :] = jnp.where(row > 0, low, 0.0)
        high = padded[stage, 2:6, 18:20, 8:24, :]
        padded[stage, 2:6, 18:20, 8:24, :] = jnp.where(row < n_row - 1, high, 0.0)

    def first_step(i, edges):
        values = [field[c, i] for c in range(6)]
        rate = rates(0, i, values)
        scale, pick = lapse[i], weighted[i]
        for c in range(6):
            value = values[c] + time_step * rate[c]
            section[c, i] = value
            masked[0, c, pl.ds(pl.multiple_of(i * ct, ct), ct), :] = value * pick
            edges = keep_product(1, c, i, scale * value, edges)
        return edges

    def second_step(i, nothing):
        values = [section[c, i] for c in range(6)]
        rate = rates(1, i, values)
        pick = weighted[i]
        for c in range(6):
            value = 0.5 * (field[c, i] + values[c] + time_step * rate[c])
            fresh[c, i] = value
            masked[1, c, pl.ds(pl.multiple_of(i * ct, ct), ct), :] = value * pick
        return nothing

    landed(pair, 0)
    mine = pl.ds(core * half, half)
    gram[mine] = gram[mine] + pair[...]
    for d in range(1, half):
        send(gram.at[core * half + lax.rem(spot + d, half)], plane.at[d - 1], in_half(d), 1)

    for copy in halos[0]:
        copy.wait_recv()
    zero_ends(0)
    keep_edges(1, lax.fori_loop(0, cr, first_step, no_edges()))
    for copy in halos[1]:
        copy.start()
    ones = jnp.ones((8, cp), jnp.float32)
    sampled_one = nt(ones, masked[0].reshape(6 * cr * ct, cp))

    landed(plane, 1)
    total = gram[owner]
    for d in range(1, half):
        total = total + plane[d - 1]
    deep[0] = total
    for d in range(1, n_th):
        send(deep.at[0], deep.at[d], along(d), 2)

    for copy in halos[1]:
        copy.wait_recv()
    zero_ends(1)
    lax.fori_loop(0, cr, second_step, 0)
    store = pltpu.make_async_copy(fresh, new_ref, store_sem)
    store.start()
    sampled_two = nt(ones, masked[1].reshape(6 * cr * ct, cp))
    width = 3 * cr * ct
    place_row = lax.broadcasted_iota(jnp.int32, (8, width), 0)
    snap = jnp.where(place_row == 4, sampled_one[:, :width], 0.0)
    snap = jnp.where(place_row == 5, sampled_one[:, width:], snap)
    snap = jnp.where(place_row == 6, sampled_two[:, :width], snap)
    snap = jnp.where(place_row == 7, sampled_two[:, width:], snap)
    snap_ref[...] = snap
    mat[248:256] = mat[248:256] + snap
    cross_plane[0] = nt(snap, mat[...])
    for d in range(1, chunks):
        send(cross_plane.at[0], cross_plane.at[d], in_plane(d), 3)

    landed(deep.at[1:], 2)
    total = deep[th]
    for a in range(1, n_th):
        total = total + deep[lax.rem(th - a + n_th, n_th)]
    full[owner] = total
    for d in range(1, half):
        send(full.at[owner], full.at[owner], in_half(d), 4)

    landed(cross_plane.at[1:], 3)
    total = cross_plane[owner]
    for a in range(1, chunks):
        total = total + cross_plane[lax.rem(owner - a + chunks, chunks)]
    cross_deep[0] = total
    for d in range(1, n_th):
        send(cross_deep.at[0], cross_deep.at[d], along(d), 5)

    landed(plane, 4)
    send(full.at[mine], full.at[mine], {"row": y * 2 + other}, 6)

    landed(cross_deep.at[1:], 5)
    total = cross_deep[th]
    for a in range(1, n_th):
        total = total + cross_deep[lax.rem(th - a + n_th, n_th)]
    cross_ref[...] = total

    landed(pair, 6)
    gram_ref[...] = full[...].reshape(gram_ref.shape)

    for stage in range(2):
        for copy in halos[stage]:
            copy.wait_send()
    left(pair, 0)
    left(plane, 1)
    left(deep.at[1:], 2)
    left(cross_plane.at[1:], 3)
    left(plane, 4)
    left(cross_deep.at[1:], 5)
    left(pair, 6)
    store.wait()


def sublane(x, k):
    return jnp.broadcast_to(x[k : k + 1], x.shape)


def eliminate(columns, x, follower=None):
    sub = lax.broadcasted_iota(jnp.int32, x.shape, 0)
    columns = list(columns)
    lows, recips, rows = [], [], []
    solved = jnp.zeros_like(x)
    for k in range(8):
        recip = lax.rsqrt(sublane(columns[k], k))
        low = columns[k] * recip
        for b in range(k + 1, 8):
            columns[b] = columns[b] - low * sublane(low, b)
        wide = jnp.tile(recip, (1, x.shape[1] // 128))
        line = sublane(x, k) * wide
        x = x - jnp.tile(low, (1, x.shape[1] // 128)) * line
        solved = jnp.where(sub == k, line, solved)
        lows.append(low)
        recips.append(recip)
        rows.append(line)
        if follower is not None:
            follower(k, recip, low, line)
    return lows, recips, rows, solved


def spread(tile, first):
    return [jnp.broadcast_to(tile[:, first + b : first + b + 1], (8, 128)) for b in range(8)]


def twice(x):
    return jnp.concatenate([x, x], axis=1)


def leaf(work, upper, inverse):
    for p in range(16):
        r0 = 8 * p
        x = work[r0 : r0 + 8]
        state = {}
        if p < 15:
            state["x"] = work[r0 + 8 : r0 + 16]
            state["e"] = spread(state["x"], r0)

        def follower(k, recip, low, line):
            mine = state["e"][k] * recip
            state["x"] = state["x"] - twice(mine) * line
            for b in range(k + 1, 8):
                state["e"][b] = state["e"][b] - mine * sublane(low, b)

        lows, recips, rows, solved = eliminate(spread(x, r0), x, follower if p < 15 else None)
        lane = lax.broadcasted_iota(jnp.int32, (8, 128), 1)
        sub = lax.broadcasted_iota(jnp.int32, (8, 128), 0)
        upper[r0 : r0 + 8] = jnp.where(lane >= sub + r0, solved[:, :128], 0.0)
        inverse[r0 : r0 + 8] = solved[:, 128:]
        if p < 15:
            work[r0 + 8 : r0 + 16] = state["x"]
        if p < 14:
            back = [None] * 8
            for q in range(7, -1, -1):
                value = rows[q]
                for a in range(q + 1, 8):
                    value = value - twice(sublane(lows[q], a)) * back[a]
                back[q] = value * twice(recips[q])
            for t in range(p + 2, 16):
                tile = work[8 * t : 8 * t + 8]
                for k, column in enumerate(spread(tile, r0)):
                    tile = tile - twice(column) * back[k]
                work[8 * t : 8 * t + 8] = tile


def solve_kernel(
    scale,
    gram_ref, cross_ref, snap_ref, old_ref, new_ref,
    out_new_ref, basis_ref, factor_ref,
    new, old, mat, work, upper, inverse, basis, padded,
    load_sem, store_sem,
):
    loads = [pltpu.make_async_copy(old_ref, old, load_sem.at[0]), pltpu.make_async_copy(new_ref, new, load_sem.at[1])]
    for load in loads:
        load.start()
    row = lax.broadcasted_iota(jnp.int32, (128, 128), 0)
    lane = lax.broadcasted_iota(jnp.int32, (128, 128), 1)
    unit = (row == lane).astype(jnp.float32)
    work[:, :128] = gram_ref[0:128, 0:128]
    work[:, 128:] = unit
    leaf(work, upper, inverse)
    factor_ref[0:128, 0:128] = upper[...] * (1.0 / scale)
    first_inverse = inverse[...]
    corner = nn(first_inverse, gram_ref[0:128, 128:256])
    factor_ref[0:128, 128:256] = corner * (1.0 / scale)
    lower_right = gram_ref[128:256, 128:256] - tn(corner, corner)
    last = (row >= 124) | (lane >= 124)
    work[:, :128] = jnp.where(last, unit, lower_right)
    work[:, 128:] = unit
    padded[0:128, 0:128] = first_inverse
    leaf(work, upper, inverse)
    second_inverse = inverse[...]
    below = -nn(second_inverse, tn(corner, padded[0:128, 0:128]))
    factor_ref[128:256, 0:128] = jnp.zeros((128, 128), jnp.float32)

    loads[0].wait()
    mat[0:248] = old[0:248]
    mat[248:252] = old[248:252]
    mat[252:256] = jnp.zeros((4, mat.shape[1]), jnp.float32)
    basis[0:128] = nn(first_inverse, mat[0:128])
    basis[128:256] = nn(second_inverse, mat[128:256]) + nn(below, mat[0:128])

    cross = cross_ref[...]
    cross_left, cross_right = cross[:, :128], cross[:, 128:]
    lane8 = lax.broadcasted_iota(jnp.int32, (8, 128), 1)
    sub8 = lax.broadcasted_iota(jnp.int32, (8, 128), 0)
    inner = jnp.where(lane8 < 124, cross_right, 0.0)
    low_left = nt(cross_left, first_inverse)
    low_right = nt(cross_left, below) + nt(inner, second_inverse)
    low_right = jnp.where(lane8 < 124, low_right, 0.0)
    padded[...] = jnp.zeros_like(padded)
    padded[120:128, 0:128] = low_left
    padded[120:128, 128:256] = low_right
    low = jnp.concatenate([low_left, low_right], axis=1)
    block = cross_right - nt(low, padded[...])
    block = jnp.where((sub8 >= 4) & (lane8 >= 124), block, jnp.where(lane8 == sub8 + 120, 1.0, 0.0))
    rest = snap_ref[...] - nn(low, basis[...])
    lows, recips, rows, solved = eliminate(spread(block, 120), jnp.concatenate([block, rest], axis=1))
    sub768 = lax.broadcasted_iota(jnp.int32, rest.shape, 0)
    basis[...] = basis[...] * scale
    basis[248:256] = jnp.where(sub768 >= 4, solved[:, 128:] * scale, basis[248:256])
    turned = padded[...].T * (1.0 / scale)
    factor_ref[0:128, 128:256] = jnp.where(lane >= 124, turned[0:128], factor_ref[0:128, 128:256])
    factor_ref[128:256, 128:256] = jnp.where(lane >= 124, turned[128:256], upper[...] * (1.0 / scale))
    ending = jnp.where(lane8 >= sub8 + 120, solved[:, :128] * (1.0 / scale), 0.0)
    factor_ref[248:256, 128:256] = jnp.where(sub8 >= 4, ending, factor_ref[248:256, 128:256])

    store = pltpu.make_async_copy(basis, basis_ref, store_sem.at[0])
    store.start()
    loads[1].wait()
    again = pltpu.make_async_copy(new, out_new_ref, store_sem.at[1])
    again.start()
    store.wait()
    again.wait()


def on_device(sizes, fields, lapse_field, excision, sample_cells, old_basis):
    n_row, n_th, n_ph = sizes
    cr, ct, cp = lapse_field.shape
    columns = old_basis.shape[1]
    f32 = jnp.float32
    half = n_row * n_ph // 2
    rows = 256 // (2 * half)
    cells = sample_cells.reshape(cr, ct)
    vmem = pltpu.VMEM
    new_fields, gram, cross, snap = pl.pallas_call(
        functools.partial(comm_kernel, sizes),
        out_shape=(
            jax.ShapeDtypeStruct(fields.shape, f32),
            jax.ShapeDtypeStruct((256, 256), f32),
            jax.ShapeDtypeStruct((8, 256), f32),
            jax.ShapeDtypeStruct((8, columns), f32),
        ),
        in_specs=[ANY] * 5,
        out_specs=(ANY, VMEM, VMEM, VMEM),
        scratch_shapes=[
            vmem(fields.shape, f32),
            vmem(lapse_field.shape, f32),
            vmem(excision.shape, jnp.int32),
            vmem(cells.shape, jnp.int32),
            vmem(old_basis.shape, f32),
            vmem((256, columns), f32),
            vmem(fields.shape, f32),
            vmem(fields.shape, f32),
            vmem(lapse_field.shape, f32),
            vmem((2, 6, cr * ct, cp), f32),
            vmem((2, 6, cr + 4, 32, cp), f32),
            vmem((2, 2, 4, 2, cr, cp), f32),
            vmem((2, 2, 4, 2, cr, cp), f32),
            vmem((2, 2, ct, cp), f32),
            vmem((2, 2, ct, cp), f32),
            vmem((2 * half, rows, 256), f32),
            vmem((2 * half, rows, 256), f32),
            vmem((half, rows, 256), f32),
            vmem((half - 1, rows, 256), f32),
            vmem((n_th, rows, 256), f32),
            vmem((2 * half, 8, 256), f32),
            vmem((n_th, 8, 256), f32),
            pltpu.SemaphoreType.DMA((5,)),
            pltpu.SemaphoreType.DMA,
            pltpu.SemaphoreType.DMA((2, 6)),
            pltpu.SemaphoreType.DMA((2, 6)),
            pltpu.SemaphoreType.DMA((7,)),
            pltpu.SemaphoreType.DMA((7,)),
        ],
        compiler_params=pltpu.CompilerParams(
            collective_id=0, has_side_effects=True, vmem_limit_bytes=48 * 1024 * 1024
        ),
        name="halo_and_gram",
    )(fields, lapse_field, excision, cells, old_basis)
    total_rows = columns * n_row * n_th * n_ph
    return pl.pallas_call(
        functools.partial(solve_kernel, math.sqrt(total_rows)),
        out_shape=(
            jax.ShapeDtypeStruct(fields.shape, f32),
            jax.ShapeDtypeStruct((256, columns), f32),
            jax.ShapeDtypeStruct((256, 256), f32),
        ),
        in_specs=[VMEM, VMEM, VMEM, ANY, ANY],
        out_specs=(ANY, ANY, VMEM),
        scratch_shapes=[
            vmem(fields.shape, f32),
            vmem(old_basis.shape, f32),
            vmem((256, columns), f32),
            vmem((128, 256), f32),
            vmem((128, 128), f32),
            vmem((128, 128), f32),
            vmem((256, columns), f32),
            vmem((128, 256), f32),
            pltpu.SemaphoreType.DMA((2,)),
            pltpu.SemaphoreType.DMA((2,)),
        ],
        compiler_params=pltpu.CompilerParams(vmem_limit_bytes=32 * 1024 * 1024),
        name="factor_and_solve",
    )(gram, cross, snap, old_basis, new_fields)


def solution(mesh):
    sizes = tuple(mesh.shape[name] for name in ("row", "th", "ph"))
    return jax.shard_map(
        functools.partial(on_device, sizes),
        mesh=mesh,
        in_specs=(
            P(None, "row", "th", "ph"),
            P("row", "th", "ph"),
            P("row", "th", "ph"),
            P("row", "th", "ph"),
            P(None, ("row", "th", "ph")),
        ),
        out_specs=(P(None, "row", "th", "ph"), P(None, ("row", "th", "ph")), P()),
        check_vma=False,
    )
```

```python
import functools
import math

import jax
import jax.numpy as jnp
from jax import lax
from jax.experimental import pallas as pl
from jax.experimental.pallas import tpu as pltpu
from jax.sharding import PartitionSpec as P

MESH = pl.DeviceIdType.MESH
LIMIT = 63 * 1024 * 1024
UNROLL = 2
HIGH = lax.Precision.HIGHEST
VMEM = pl.BlockSpec(memory_space=pltpu.VMEM)
HBM = pl.BlockSpec(memory_space=pltpu.HBM)

damping_rate = 3.0
time_step = 0.3
azimuth_gain = 5.0

SLOT = {0: 0, 3: 1, 2: 2, 5: 3, 1: 4, 4: 5}
EDGE = {0: 0, 3: 1, 1: 2, 4: 3}


def nt(a, b):
    return lax.dot_general(a, b, (((1,), (1,)), ((), ())), precision=HIGH, preferred_element_type=jnp.float32)


def nn(a, b):
    return lax.dot_general(a, b, (((1,), (0,)), ((), ())), precision=HIGH, preferred_element_type=jnp.float32)


def tn(a, b):
    return lax.dot_general(a, b, (((0,), (0,)), ((), ())), precision=HIGH, preferred_element_type=jnp.float32)


def diff(near_high, near_low, far_high, far_low, gain):
    return (8.0 * (near_high - near_low) - (far_high - far_low)) * (gain / 12.0)


def sublane(x, k):
    return jnp.broadcast_to(x[k : k + 1], x.shape)


def eliminate(columns, x, follower=None):
    sub = lax.broadcasted_iota(jnp.int32, x.shape, 0)
    columns = list(columns)
    lows, recips, rows = [], [], []
    solved = jnp.zeros_like(x)
    for k in range(8):
        recip = lax.rsqrt(sublane(columns[k], k))
        low = columns[k] * recip
        for b in range(k + 1, 8):
            columns[b] = columns[b] - low * sublane(low, b)
        wide = jnp.tile(recip, (1, x.shape[1] // 128))
        line = sublane(x, k) * wide
        x = x - jnp.tile(low, (1, x.shape[1] // 128)) * line
        solved = jnp.where(sub == k, line, solved)
        lows.append(low)
        recips.append(recip)
        rows.append(line)
        if follower is not None:
            follower(k, recip, low, line)
    return lows, recips, rows, solved


def spread(tile, first):
    return [jnp.broadcast_to(tile[:, first + b : first + b + 1], (8, 128)) for b in range(8)]


def twice(x):
    return jnp.concatenate([x, x], axis=1)


def leaf(work, upper, inverse):
    for p in range(16):
        r0 = 8 * p
        x = work[r0 : r0 + 8]
        state = {}
        if p < 15:
            state["x"] = work[r0 + 8 : r0 + 16]
            state["e"] = spread(state["x"], r0)

        def follower(k, recip, low, line):
            mine = state["e"][k] * recip
            state["x"] = state["x"] - twice(mine) * line
            for b in range(k + 1, 8):
                state["e"][b] = state["e"][b] - mine * sublane(low, b)

        lows, recips, rows, solved = eliminate(spread(x, r0), x, follower if p < 15 else None)
        lane = lax.broadcasted_iota(jnp.int32, (8, 128), 1)
        sub = lax.broadcasted_iota(jnp.int32, (8, 128), 0)
        upper[r0 : r0 + 8] = jnp.where(lane >= sub + r0, solved[:, :128], 0.0)
        inverse[r0 : r0 + 8] = solved[:, 128:]
        if p < 15:
            work[r0 + 8 : r0 + 16] = state["x"]
        if p < 14:
            back = [None] * 8
            for q in range(7, -1, -1):
                value = rows[q]
                for a in range(q + 1, 8):
                    value = value - twice(sublane(lows[q], a)) * back[a]
                back[q] = value * twice(recips[q])
            for t in range(p + 2, 16):
                tile = work[8 * t : 8 * t + 8]
                for k, column in enumerate(spread(tile, r0)):
                    tile = tile - twice(column) * back[k]
                work[8 * t : 8 * t + 8] = tile


def comm_kernel(
    sizes, scale,
    fields_ref, lapse_ref, excision_ref, cells_ref, old_ref,
    new_ref, inverse_ref, factor_ref, matrix_ref,
    field, lapse, excision, cells, old, mat, fresh, section, weighted, masked0, masked1,
    padded0, padded1, polar_out0, polar_out1, polar_in0, polar_in1, edge_out0, edge_out1, edge_in0, edge_in1,
    gram, full, pair, plane, deep, cross_pair, cross_plane, cross_deep, inv, fac,
    work, factor_block, upper, inverse, padded_low,
    load_sem, store_sem, halo_send, halo_recv, send_sem, recv_sem,
):
    masked, padded = (masked0, masked1), (padded0, padded1)
    polar_out, polar_in = (polar_out0, polar_out1), (polar_in0, polar_in1)
    edge_out, edge_in = (edge_out0, edge_out1), (edge_in0, edge_in1)
    n_row, n_th, n_ph = sizes
    n_y = n_row // 2
    row, th, ph = lax.axis_index("row"), lax.axis_index("th"), lax.axis_index("ph")
    core, y = lax.rem(row, 2), lax.div(row, 2)
    spot = y * n_ph + ph
    half = n_y * n_ph
    chunks = 2 * half
    owner = core * half + spot
    cr, ct, cp = 16, 16, 128

    loads = [
        pltpu.make_async_copy(source, target, load_sem.at[k])
        for k, (source, target) in enumerate(
            ((old_ref, old), (fields_ref, field), (lapse_ref, lapse), (excision_ref, excision), (cells_ref, cells))
        )
    ]
    for load in loads:
        load.start()

    def place(index):
        which, rest = lax.div(index, half), lax.rem(index, half)
        return {"row": lax.div(rest, n_ph) * 2 + which, "ph": lax.rem(rest, n_ph)}

    def in_plane(d):
        return place(lax.rem(owner + d, chunks))

    def in_half(d):
        return place(core * half + lax.rem(spot + d, half))

    def along(d):
        return {"th": lax.rem(th + d, n_th)}

    barrier = pltpu.get_barrier_semaphore()
    for d in range(1, chunks):
        pl.semaphore_signal(barrier, inc=1, device_id=in_plane(d), device_id_type=MESH)
    for d in range(1, n_th):
        pl.semaphore_signal(barrier, inc=1, device_id=along(d), device_id_type=MESH)

    def send(source, target, device, k):
        copy = pltpu.make_async_remote_copy(
            src_ref=source, dst_ref=target, send_sem=send_sem.at[k], recv_sem=recv_sem.at[k],
            device_id=device, device_id_type=MESH,
        )
        copy.start()

    def landed(ref, k):
        pltpu.make_async_copy(ref, ref, recv_sem.at[k]).wait()

    def left(ref, k):
        pltpu.make_async_copy(ref, ref, send_sem.at[k]).wait()

    lane = lax.broadcasted_iota(jnp.int32, (ct, cp), 1)
    lane_pair = lax.shift_right_logical(lane, 1)

    loads[0].wait()
    mat[0:248] = old[0:248]
    mat[248:252] = old[248:252]
    mat[252:256] = jnp.zeros((4, mat.shape[1]), jnp.float32)
    top = nt(mat[0:128], mat[0:128])
    top = jnp.concatenate([top, jnp.zeros_like(top)], axis=1)
    gram_rows = gram.shape[1]
    gram[0:half] = top.reshape(half, gram_rows, 256)
    gram[half : 2 * half] = nt(mat[128:256], mat[...]).reshape(half, gram_rows, 256)
    pl.semaphore_wait(barrier, chunks - 1 + n_th - 1)
    other = 1 - core
    send(gram.at[pl.ds(other * half, half)], pair, {"row": y * 2 + other}, 0)

    def keep_product(stage, c, i, value, edges):
        slot = SLOT[c]
        padded[stage][slot, i + 2, 8:24, :] = value
        if slot < 4:
            for s in range(2):
                polar_out[stage][0, slot, s, pl.ds(i, 1), :] = value[s : s + 1]
                polar_out[stage][1, slot, s, pl.ds(i, 1), :] = value[14 + s : 15 + s]
        if c in EDGE:
            t = EDGE[c] * cr + i
            here = lane_pair == t
            edges = (
                jnp.where(here, pltpu.roll(value, 2 * t, 1), edges[0]),
                jnp.where(here, pltpu.roll(value, (2 * t + 2) % cp, 1), edges[1]),
            )
        return edges

    def unrolled(body, carry, by=UNROLL):
        def several(k, carry):
            for u in range(by):
                carry = body(k * by + u, carry)
            return carry

        if by == cr:
            return several(0, carry)
        return lax.fori_loop(0, cr // by, several, carry)

    def sample(stage):
        for c in range(6):
            for h in range(cr * ct // cp):
                line = jnp.sum(masked[stage][c, h * cp : (h + 1) * cp, :].T, axis=0, keepdims=True)
                r, first = 252 + 2 * stage + c // 3, (c % 3) * cr * ct + h * cp
                mat[r : r + 1, first : first + cp] = line

    def at(i):
        return slice(i * ct, (i + 1) * ct) if isinstance(i, int) else pl.ds(pl.multiple_of(i * ct, ct), ct)

    def no_edges():
        return jnp.zeros((ct, cp), jnp.float32), jnp.zeros((ct, cp), jnp.float32)

    def first_products(i, edges):
        scale = lapse[i]
        for c in range(6):
            edges = keep_product(0, c, i, scale * field[c, i], edges)
        return edges

    def halo_copies(stage):
        rows = ((padded[stage].at[2:6, 2:4, 8:24, :], padded[stage].at[2:6, 18:20, 8:24, :], {"row": lax.rem(row + n_row - 1, n_row)}),
                (padded[stage].at[2:6, 16:18, 8:24, :], padded[stage].at[2:6, 0:2, 8:24, :], {"row": lax.rem(row + 1, n_row)}))
        polars = ((polar_out[stage].at[0], polar_in[stage].at[1], {"th": lax.rem(th + n_th - 1, n_th)}),
                  (polar_out[stage].at[1], polar_in[stage].at[0], {"th": lax.rem(th + 1, n_th)}))
        edges = ((edge_out[stage].at[0], edge_in[stage].at[1], {"ph": lax.rem(ph + n_ph - 1, n_ph)}),
                 (edge_out[stage].at[1], edge_in[stage].at[0], {"ph": lax.rem(ph + 1, n_ph)}))
        return [
            pltpu.make_async_remote_copy(
                src_ref=source, dst_ref=target, send_sem=halo_send.at[stage, k], recv_sem=halo_recv.at[stage, k],
                device_id=device, device_id_type=MESH,
            )
            for k, (source, target, device) in enumerate(rows + polars + edges)
        ]

    def keep_edges(stage, edges):
        edge_out[stage][0] = edges[0]
        edge_out[stage][1] = edges[1]

    for load in loads[1:]:
        load.wait()
    keep_edges(0, unrolled(first_products, no_edges(), cr))

    halos = [halo_copies(0), halo_copies(1)]
    for copy in halos[0]:
        copy.start()
    pol_index = (th * ct + lax.broadcasted_iota(jnp.int32, (ct, cp), 0)).astype(jnp.float32)
    polar = jnp.pi * (pol_index + 0.5) / (n_th * ct)
    polar_weight = jnp.sqrt(jnp.sin(polar))
    chosen = cells[...].T
    for i in range(cr):
        radius = 1.0 + 2.0 * ((row * cr + i).astype(jnp.float32) + 0.5) / (n_row * cr)
        weighted[i] = jnp.where(lane == chosen[:, i : i + 1], polar_weight * radius, 0.0)

    def rates(stage, i, c_values):
        damped = damping_rate * excision[i].astype(jnp.float32)
        lo_edge, hi_edge = edge_in[stage][0], edge_in[stage][1]
        for slot in range(4):
            for s in range(2):
                low = polar_in[stage][0, slot, s, pl.ds(i, 1), :]
                high = polar_in[stage][1, slot, s, pl.ds(i, 1), :]
                padded[stage][slot, i + 2, 6 + s : 7 + s, :] = jnp.where(th > 0, low, 0.0)
                padded[stage][slot, i + 2, 24 + s : 25 + s, :] = jnp.where(th < n_th - 1, high, 0.0)

        def rad(c):
            get = lambda o: padded[stage][SLOT[c], i + 2 + o, 8:24, :]
            return diff(get(1), get(-1), get(2), get(-2), 1.0)

        def pol(c):
            get = lambda o: padded[stage][SLOT[c], i + 2, 8 + o : 24 + o, :]
            return diff(get(1), get(-1), get(2), get(-2), 1.0)

        def azi(c):
            here = padded[stage][SLOT[c], i + 2, 8:24, :]
            t = EDGE[c] * cr + i
            low = pltpu.roll(lo_edge, cp - 2 - 2 * t, 1)
            high = pltpu.roll(hi_edge, (cp - 2 * t) % cp, 1)
            far_low = pltpu.roll(jnp.where(lane >= cp - 2, low, here), 2, 1)
            near_low = pltpu.roll(jnp.where(lane >= cp - 1, low, here), 1, 1)
            near_high = pltpu.roll(jnp.where(lane < 1, high, here), cp - 1, 1)
            far_high = pltpu.roll(jnp.where(lane < 2, high, here), cp - 2, 1)
            return diff(near_high, near_low, far_high, far_low, azimuth_gain)

        out = []
        for start, sign in ((3, 1.0), (0, -1.0)):
            curls = (pol(start + 2) - azi(start + 1), azi(start) - rad(start + 2), rad(start + 1) - pol(start))
            for k in range(3):
                c = len(out)
                out.append((curls[k] if sign > 0 else -curls[k]) - damped * c_values[c])
        return out

    def zero_ends(stage):
        low = padded[stage][2:6, 0:2, 8:24, :]
        padded[stage][2:6, 0:2, 8:24, :] = jnp.where(row > 0, low, 0.0)
        high = padded[stage][2:6, 18:20, 8:24, :]
        padded[stage][2:6, 18:20, 8:24, :] = jnp.where(row < n_row - 1, high, 0.0)

    def first_step(i, edges):
        values = [field[c, i] for c in range(6)]
        rate = rates(0, i, values)
        scale, pick = lapse[i], weighted[i]
        for c in range(6):
            value = values[c] + time_step * rate[c]
            section[c, i] = value
            masked[0][c, at(i), :] = value * pick
            edges = keep_product(1, c, i, scale * value, edges)
        return edges

    def second_step(i, nothing):
        values = [section[c, i] for c in range(6)]
        rate = rates(1, i, values)
        pick = weighted[i]
        for c in range(6):
            value = 0.5 * (field[c, i] + values[c] + time_step * rate[c])
            fresh[c, i] = value
            masked[1][c, at(i), :] = value * pick
        return nothing

    landed(pair, 0)
    mine = pl.ds(core * half, half)
    gram[mine] = gram[mine] + pair[...]
    for d in range(1, half):
        send(gram.at[core * half + lax.rem(spot + d, half)], plane.at[d - 1], in_half(d), 1)

    for copy in halos[0]:
        copy.wait_recv()
    zero_ends(0)
    keep_edges(1, unrolled(first_step, no_edges()))
    for copy in halos[1]:
        copy.start()
    sample(0)

    landed(plane, 1)
    total = gram[owner]
    for d in range(1, half):
        total = total + plane[d - 1]
    deep[0] = total
    for d in range(1, n_th):
        send(deep.at[0], deep.at[d], along(d), 2)

    for copy in halos[1]:
        copy.wait_recv()
    zero_ends(1)
    unrolled(second_step, 0)
    landed(deep.at[1:], 2)
    total = deep[th]
    for a in range(1, n_th):
        total = total + deep[lax.rem(th - a + n_th, n_th)]
    full[owner] = total
    for d in range(1, half):
        send(full.at[owner], full.at[owner], in_half(d), 4)

    stores = [pltpu.make_async_copy(fresh, new_ref, store_sem.at[0])]
    stores[0].start()
    sample(1)
    stores.append(pltpu.make_async_copy(mat, matrix_ref, store_sem.at[1]))
    stores[1].start()
    place_row = lax.broadcasted_iota(jnp.int32, (8, mat.shape[1]), 0)
    snap = jnp.where(place_row >= 4, mat[248:256], 0.0)
    cross_pair[core] = nt(snap, mat[...])[4:8]
    send(cross_pair.at[core], cross_pair.at[core], {"row": y * 2 + other}, 3)
    landed(cross_pair.at[0], 3)
    cross_plane[0] = cross_pair[0] + cross_pair[1]
    for d in range(1, half):
        send(cross_plane.at[0], cross_plane.at[d], in_half(d), 7)

    landed(plane, 4)
    send(full.at[mine], full.at[mine], {"row": y * 2 + other}, 6)
    square = lax.broadcasted_iota(jnp.int32, (128, 128), 0)
    column = lax.broadcasted_iota(jnp.int32, (128, 128), 1)
    unit = (square == column).astype(jnp.float32)
    inv[0:128, 128:256] = jnp.zeros((128, 128), jnp.float32)
    fac[128:256, 0:128] = jnp.zeros((128, 128), jnp.float32)
    padded_low[...] = jnp.zeros_like(padded_low)
    landed(pair, 6)
    gram_half = chunks // 2
    top = full[0:gram_half].reshape(128, 256)
    bottom = full[gram_half:chunks].reshape(128, 256)
    work[:, :128] = top[:, :128]
    work[:, 128:] = unit
    upper[...] = bottom[:, :128]

    def block(b, nothing):
        leaf(work, factor_block, inverse)

        @pl.when(b == 0)
        def _():
            first = inverse[...]
            inv[0:128, 0:128] = first
            fac[0:128, 0:128] = factor_block[...] * (1.0 / scale)
            corner = nt(first, upper[...])
            upper[...] = corner
            last = (square >= 124) | (column >= 124)
            right = full[gram_half:chunks].reshape(128, 256)[:, 128:]
            work[:, :128] = jnp.where(last, unit, right - tn(corner, corner))
            work[:, 128:] = unit
            landed(cross_plane.at[1:], 7)
            total = cross_plane[spot]
            for a in range(1, half):
                total = total + cross_plane[lax.rem(spot - a + half, half)]
            cross_deep[0] = total
            for d in range(1, n_th):
                send(cross_deep.at[0], cross_deep.at[d], along(d), 5)

        return nothing

    lax.fori_loop(0, 2, block, 0)

    second = inverse[...]
    first = inv[0:128, 0:128]
    corner = upper[...]
    below = -nn(second, tn(corner, first))
    inv[128:256, 0:128] = below
    inv[128:256, 128:256] = second

    landed(cross_deep.at[1:], 5)
    cross = cross_deep[th]
    for a in range(1, n_th):
        cross = cross + cross_deep[lax.rem(th - a + n_th, n_th)]
    cross = jnp.concatenate([jnp.zeros((4, 256), jnp.float32), cross], axis=0)
    cross_left, cross_right = cross[:, :128], cross[:, 128:]
    lane8 = lax.broadcasted_iota(jnp.int32, (8, 128), 1)
    sub8 = lax.broadcasted_iota(jnp.int32, (8, 128), 0)
    inner = jnp.where(lane8 < 124, cross_right, 0.0)
    low_left = nt(cross_left, first)
    low_right = jnp.where(lane8 < 124, nt(cross_left, below) + nt(inner, second), 0.0)
    padded_low[120:128, 0:128] = low_left
    padded_low[120:128, 128:256] = low_right
    low = jnp.concatenate([low_left, low_right], axis=1)
    snapshot_block = cross_right - nt(low, padded_low[...])
    real = sub8 >= 4
    diagonal = (lane8 == sub8 + 120).astype(jnp.float32)
    snapshot_block = jnp.where(real & (lane8 >= 124), snapshot_block, diagonal)
    rest_left = -(nn(low_left, first) + nn(low_right, below))
    rest_right = diagonal - nn(low_right, second)
    _, _, _, solved = eliminate(
        spread(snapshot_block, 120), jnp.concatenate([snapshot_block, rest_left, rest_right], axis=1)
    )
    real_wide = lax.broadcasted_iota(jnp.int32, (8, 256), 0) >= 4
    inv[248:256] = jnp.where(real_wide, solved[:, 128:], inv[248:256])
    turned = padded_low[...].T
    fac[0:128, 128:256] = jnp.where(column >= 124, turned[0:128], corner) * (1.0 / scale)
    fac[128:256, 128:256] = jnp.where(column >= 124, turned[128:256], factor_block[...]) * (1.0 / scale)
    finish = jnp.where(lane8 >= sub8 + 120, solved[:, :128] * (1.0 / scale), 0.0)
    fac[248:256, 128:256] = jnp.where(real, finish, fac[248:256, 128:256])

    stores.append(pltpu.make_async_copy(inv, inverse_ref, store_sem.at[2]))
    stores.append(pltpu.make_async_copy(fac, factor_ref, store_sem.at[3]))
    for store in stores[2:]:
        store.start()
    for stage in range(2):
        for copy in halos[stage]:
            copy.wait_send()
    left(pair, 0)
    left(plane, 1)
    left(deep.at[1:], 2)
    left(cross_pair.at[0], 3)
    left(cross_plane.at[1:], 7)
    left(plane, 4)
    left(cross_deep.at[1:], 5)
    left(pair, 6)
    for store in stores:
        store.wait()


def apply_kernel(
    scale,
    new_ref, inverse_ref, factor_ref, matrix_ref,
    out_new_ref, basis_ref, out_factor_ref,
    inverse, matrix, new, factor, basis, load_sem, sem,
):
    def pieces(source, target, count):
        rows = source.shape[0] // count
        return [(source.at[k * rows : (k + 1) * rows], target.at[k * rows : (k + 1) * rows]) for k in range(count)]

    loads = pieces(inverse_ref, inverse, 2) + pieces(matrix_ref, matrix, 2) + [(factor_ref, factor), (new_ref, new)]
    loads = [pltpu.make_async_copy(source, target, load_sem.at[k]) for k, (source, target) in enumerate(loads)]
    for load in loads:
        load.start()
    copies = []
    for h in range(2):
        rows = slice(128 * h, 128 * h + 128)
        loads[h].wait()
        loads[2 + h].wait()
        basis[rows] = nn(inverse[rows, : 128 * h + 128], matrix[: 128 * h + 128]) * scale
        copies.append(pltpu.make_async_copy(basis.at[rows], basis_ref.at[rows], sem.at[h]))
        copies[-1].start()
        if h == 0:
            for k, source, target in ((4, factor, out_factor_ref), (5, new, out_new_ref)):
                loads[k].wait()
                copies.append(pltpu.make_async_copy(source, target, sem.at[k - 2]))
                copies[-1].start()
    for copy in copies:
        copy.wait()


def on_device(sizes, fields, lapse_field, excision, sample_cells, old_basis):
    n_row, n_th, n_ph = sizes
    cr, ct, cp = lapse_field.shape
    columns = old_basis.shape[1]
    f32 = jnp.float32
    half = n_row * n_ph // 2
    rows = 256 // (2 * half)
    cells = sample_cells.reshape(cr, ct)
    vmem = pltpu.VMEM
    scale = math.sqrt(columns * n_row * n_th * n_ph)
    between = (
        jax.ShapeDtypeStruct(fields.shape, f32),
        jax.ShapeDtypeStruct((256, 256), f32),
        jax.ShapeDtypeStruct((256, 256), f32),
        jax.ShapeDtypeStruct((256, columns), f32),
    )
    between = pl.pallas_call(
        functools.partial(comm_kernel, sizes, scale),
        out_shape=between,
        in_specs=[HBM] * 5,
        out_specs=(HBM,) * 4,
        scratch_shapes=[
            vmem(fields.shape, f32),
            vmem(lapse_field.shape, f32),
            vmem(excision.shape, jnp.int32),
            vmem(cells.shape, jnp.int32),
            vmem(old_basis.shape, f32),
            vmem((256, columns), f32),
            vmem(fields.shape, f32),
            vmem(fields.shape, f32),
            vmem(lapse_field.shape, f32),
            vmem((6, cr * ct, cp), f32),
            vmem((6, cr * ct, cp), f32),
            vmem((6, cr + 4, 32, cp), f32),
            vmem((6, cr + 4, 32, cp), f32),
            vmem((2, 4, 2, cr, cp), f32),
            vmem((2, 4, 2, cr, cp), f32),
            vmem((2, 4, 2, cr, cp), f32),
            vmem((2, 4, 2, cr, cp), f32),
            vmem((2, ct, cp), f32),
            vmem((2, ct, cp), f32),
            vmem((2, ct, cp), f32),
            vmem((2, ct, cp), f32),
            vmem((2 * half, rows, 256), f32),
            vmem((2 * half, rows, 256), f32),
            vmem((half, rows, 256), f32),
            vmem((half - 1, rows, 256), f32),
            vmem((n_th, rows, 256), f32),
            vmem((2, 4, 256), f32),
            vmem((half, 4, 256), f32),
            vmem((n_th, 4, 256), f32),
            vmem((256, 256), f32),
            vmem((256, 256), f32),
            vmem((128, 256), f32),
            vmem((128, 128), f32),
            vmem((128, 128), f32),
            vmem((128, 128), f32),
            vmem((128, 256), f32),
            pltpu.SemaphoreType.DMA((5,)),
            pltpu.SemaphoreType.DMA((4,)),
            pltpu.SemaphoreType.DMA((2, 6)),
            pltpu.SemaphoreType.DMA((2, 6)),
            pltpu.SemaphoreType.DMA((8,)),
            pltpu.SemaphoreType.DMA((8,)),
        ],
        compiler_params=pltpu.CompilerParams(
            collective_id=0, has_side_effects=True, vmem_limit_bytes=LIMIT
        ),
        name="halo_and_gram",
    )(fields, lapse_field, excision, cells, old_basis)
    return pl.pallas_call(
        functools.partial(apply_kernel, scale),
        out_shape=(
            jax.ShapeDtypeStruct(fields.shape, f32),
            jax.ShapeDtypeStruct((256, columns), f32),
            jax.ShapeDtypeStruct((256, 256), f32),
        ),
        in_specs=[HBM] * 4,
        out_specs=(HBM,) * 3,
        scratch_shapes=[
            vmem((256, 256), f32),
            vmem((256, columns), f32),
            vmem(fields.shape, f32),
            vmem((256, 256), f32),
            vmem((256, columns), f32),
            pltpu.SemaphoreType.DMA((6,)),
            pltpu.SemaphoreType.DMA((4,)),
        ],
        compiler_params=pltpu.CompilerParams(vmem_limit_bytes=LIMIT),
        name="apply",
    )(*between)


def solution(mesh):
    sizes = tuple(mesh.shape[name] for name in ("row", "th", "ph"))
    return jax.shard_map(
        functools.partial(on_device, sizes),
        mesh=mesh,
        in_specs=(
            P(None, "row", "th", "ph"),
            P("row", "th", "ph"),
            P("row", "th", "ph"),
            P("row", "th", "ph"),
            P(None, ("row", "th", "ph")),
        ),
        out_specs=(P(None, "row", "th", "ph"), P(None, ("row", "th", "ph")), P()),
        check_vma=False,
    )
```

```python
import functools
import math

import jax
import jax.numpy as jnp
from jax import lax
from jax.experimental import pallas as pl
from jax.experimental.pallas import tpu as pltpu
from jax.sharding import PartitionSpec as P

MESH = pl.DeviceIdType.MESH
LIMIT = 63 * 1024 * 1024
UNROLL = 2
HIGH = lax.Precision.HIGHEST
HBM = pl.BlockSpec(memory_space=pltpu.HBM)

damping_rate = 3.0
time_step = 0.3
azimuth_gain = 5.0

SLOT = {0: 0, 3: 1, 2: 2, 5: 3, 1: 4, 4: 5}
EDGE = {0: 0, 3: 1, 1: 2, 4: 3}


def nt(a, b):
    return lax.dot_general(a, b, (((1,), (1,)), ((), ())), precision=HIGH, preferred_element_type=jnp.float32)


def nn(a, b):
    return lax.dot_general(a, b, (((1,), (0,)), ((), ())), precision=HIGH, preferred_element_type=jnp.float32)


def tn(a, b):
    return lax.dot_general(a, b, (((0,), (0,)), ((), ())), precision=HIGH, preferred_element_type=jnp.float32)


def diff(near_high, near_low, far_high, far_low, gain):
    return (8.0 * (near_high - near_low) - (far_high - far_low)) * (gain / 12.0)


def sublane(x, k):
    return jnp.broadcast_to(x[k : k + 1], x.shape)


def eliminate(columns, x, follower=None):
    sub = lax.broadcasted_iota(jnp.int32, x.shape, 0)
    columns = list(columns)
    lows, recips, rows = [], [], []
    solved = jnp.zeros_like(x)
    for k in range(8):
        recip = lax.rsqrt(sublane(columns[k], k))
        low = columns[k] * recip
        for b in range(k + 1, 8):
            columns[b] = columns[b] - low * sublane(low, b)
        wide = jnp.tile(recip, (1, x.shape[1] // 128))
        line = sublane(x, k) * wide
        x = x - jnp.tile(low, (1, x.shape[1] // 128)) * line
        solved = jnp.where(sub == k, line, solved)
        lows.append(low)
        recips.append(recip)
        rows.append(line)
        if follower is not None:
            follower(k, recip, low, line)
    return lows, recips, rows, solved


def spread(tile, first):
    return [jnp.broadcast_to(tile[:, first + b : first + b + 1], (8, 128)) for b in range(8)]


def twice(x):
    return jnp.concatenate([x, x], axis=1)


def leaf(work, upper, inverse):
    for p in range(16):
        r0 = 8 * p
        x = work[r0 : r0 + 8]
        state = {}
        if p < 15:
            state["x"] = work[r0 + 8 : r0 + 16]
            state["e"] = spread(state["x"], r0)

        def follower(k, recip, low, line):
            mine = state["e"][k] * recip
            state["x"] = state["x"] - twice(mine) * line
            for b in range(k + 1, 8):
                state["e"][b] = state["e"][b] - mine * sublane(low, b)

        lows, recips, rows, solved = eliminate(spread(x, r0), x, follower if p < 15 else None)
        lane = lax.broadcasted_iota(jnp.int32, (8, 128), 1)
        sub = lax.broadcasted_iota(jnp.int32, (8, 128), 0)
        upper[r0 : r0 + 8] = jnp.where(lane >= sub + r0, solved[:, :128], 0.0)
        inverse[r0 : r0 + 8] = solved[:, 128:]
        if p < 15:
            work[r0 + 8 : r0 + 16] = state["x"]
        if p < 14:
            back = [None] * 8
            for q in range(7, -1, -1):
                value = rows[q]
                for a in range(q + 1, 8):
                    value = value - twice(sublane(lows[q], a)) * back[a]
                back[q] = value * twice(recips[q])
            for t in range(p + 2, 16):
                tile = work[8 * t : 8 * t + 8]
                for k, column in enumerate(spread(tile, r0)):
                    tile = tile - twice(column) * back[k]
                work[8 * t : 8 * t + 8] = tile


def comm_kernel(
    sizes, scale,
    fields_ref, lapse_ref, excision_ref, cells_ref, old_ref,
    new_ref, basis_ref, factor_ref,
    field, lapse, excision, cells, old, mat, fresh, section, weighted, masked0, masked1,
    padded0, padded1, polar_out0, polar_out1, polar_in0, polar_in1, edge_out0, edge_out1, edge_in0, edge_in1, outside,
    first_part, first_pair, first_sum, first_plane, first_deep, first_full,
    other_part, other_pair, other_sum, other_plane, other_deep, other_full,
    cross_plane, cross_deep,
    work, upper, inverse, padded_low, basis, factor,
    load_sem, store_sem, halo_send, halo_recv, send_sem, recv_sem,
):
    masked, padded = (masked0, masked1), (padded0, padded1)
    polar_out, polar_in = (polar_out0, polar_out1), (polar_in0, polar_in1)
    edge_out, edge_in = (edge_out0, edge_out1), (edge_in0, edge_in1)
    n_row, n_th, n_ph = sizes
    n_y = n_row // 2
    row, th, ph = lax.axis_index("row"), lax.axis_index("th"), lax.axis_index("ph")
    core, y = lax.rem(row, 2), lax.div(row, 2)
    spot = y * n_ph + ph
    half = n_y * n_ph
    chunks = 2 * half
    owner = core * half + spot
    cr, ct, cp = 16, 16, 128

    loads = [
        pltpu.make_async_copy(source, target, load_sem.at[k])
        for k, (source, target) in enumerate(
            ((old_ref, old), (fields_ref, field), (lapse_ref, lapse), (excision_ref, excision), (cells_ref, cells))
        )
    ]
    for load in loads:
        load.start()

    def place(index):
        which, rest = lax.div(index, half), lax.rem(index, half)
        return {"row": lax.div(rest, n_ph) * 2 + which, "ph": lax.rem(rest, n_ph)}

    def in_plane(d):
        return place(lax.rem(owner + d, chunks))

    def in_half(d):
        return place(core * half + lax.rem(spot + d, half))

    def along(d):
        return {"th": lax.rem(th + d, n_th)}

    barrier = pltpu.get_barrier_semaphore()
    for d in range(1, chunks):
        pl.semaphore_signal(barrier, inc=1, device_id=in_plane(d), device_id_type=MESH)
    for d in range(1, n_th):
        pl.semaphore_signal(barrier, inc=1, device_id=along(d), device_id_type=MESH)

    def send(source, target, device, k):
        copy = pltpu.make_async_remote_copy(
            src_ref=source, dst_ref=target, send_sem=send_sem.at[k], recv_sem=recv_sem.at[k],
            device_id=device, device_id_type=MESH,
        )
        copy.start()

    def landed(ref, k):
        pltpu.make_async_copy(ref, ref, recv_sem.at[k]).wait()

    def left(ref, k):
        pltpu.make_async_copy(ref, ref, send_sem.at[k]).wait()

    lane = lax.broadcasted_iota(jnp.int32, (ct, cp), 1)
    lane_pair = lax.shift_right_logical(lane, 1)

    loads[0].wait()
    mat[0:248] = old[0:248]
    mat[248:252] = old[248:252]
    mat[252:256] = jnp.zeros((4, mat.shape[1]), jnp.float32)
    tiles = first_part.shape
    first_part[...] = nt(mat[0:128], mat[0:128]).reshape(tiles)
    pl.semaphore_wait(barrier, chunks - 1 + n_th - 1)
    other = 1 - core
    send(first_part, first_pair, {"row": y * 2 + other}, 0)

    def keep_product(stage, c, i, value):
        slot = SLOT[c]
        padded[stage][slot, i + 2, 8:24, :] = value
        if slot < 4:
            for s in range(2):
                polar_out[stage][0, slot, s, pl.ds(i, 1), :] = value[s : s + 1]
                polar_out[stage][1, slot, s, pl.ds(i, 1), :] = value[14 + s : 15 + s]

    def keep_edges(stage):
        low = high = jnp.zeros((ct, cp), jnp.float32)
        for c, e in EDGE.items():
            for i in range(cr):
                t = e * cr + i
                value = padded[stage][SLOT[c], i + 2, 8:24, :]
                here = lane_pair == t
                low = jnp.where(here, pltpu.roll(value, 2 * t, 1), low)
                high = jnp.where(here, pltpu.roll(value, (2 * t + 2) % cp, 1), high)
        edge_out[stage][0] = low
        edge_out[stage][1] = high

    def beyond(stage):
        low, high = edge_in[stage][0], edge_in[stage][1]
        for e in range(4):
            for i in range(cr):
                t = e * cr + i
                moved = pltpu.roll(high, (cp - 2 * t) % cp, 1), pltpu.roll(low, cp - 2 - 2 * t, 1)
                outside[e, i] = jnp.where(lane < cp // 2, *moved)

    def unrolled(body, carry, by=UNROLL):
        def several(k, carry):
            for u in range(by):
                carry = body(k * by + u, carry)
            return carry

        if by == cr:
            return several(0, carry)
        return lax.fori_loop(0, cr // by, several, carry)

    def sample(stage):
        for c in range(6):
            for h in range(cr * ct // cp):
                line = jnp.sum(masked[stage][c, h * cp : (h + 1) * cp, :].T, axis=0, keepdims=True)
                r, first = 252 + 2 * stage + c // 3, (c % 3) * cr * ct + h * cp
                mat[r : r + 1, first : first + cp] = line

    def at(i):
        return slice(i * ct, (i + 1) * ct) if isinstance(i, int) else pl.ds(pl.multiple_of(i * ct, ct), ct)

    def first_products(i, nothing):
        gain = lapse[i]
        for c in range(6):
            keep_product(0, c, i, gain * field[c, i])
        return nothing

    def halo_copies(stage):
        rows = ((padded[stage].at[2:6, 2:4, 8:24, :], padded[stage].at[2:6, 18:20, 8:24, :], {"row": lax.rem(row + n_row - 1, n_row)}),
                (padded[stage].at[2:6, 16:18, 8:24, :], padded[stage].at[2:6, 0:2, 8:24, :], {"row": lax.rem(row + 1, n_row)}))
        polars = ((polar_out[stage].at[0], polar_in[stage].at[1], {"th": lax.rem(th + n_th - 1, n_th)}),
                  (polar_out[stage].at[1], polar_in[stage].at[0], {"th": lax.rem(th + 1, n_th)}))
        edges = ((edge_out[stage].at[0], edge_in[stage].at[1], {"ph": lax.rem(ph + n_ph - 1, n_ph)}),
                 (edge_out[stage].at[1], edge_in[stage].at[0], {"ph": lax.rem(ph + 1, n_ph)}))
        return [
            pltpu.make_async_remote_copy(
                src_ref=source, dst_ref=target, send_sem=halo_send.at[stage, k], recv_sem=halo_recv.at[stage, k],
                device_id=device, device_id_type=MESH,
            )
            for k, (source, target, device) in enumerate(rows + polars + edges)
        ]

    for load in loads[1:]:
        load.wait()
    unrolled(first_products, 0, cr)
    keep_edges(0)

    halos = [halo_copies(0), halo_copies(1)]
    for copy in halos[0]:
        copy.start()
    pol_index = (th * ct + lax.broadcasted_iota(jnp.int32, (ct, cp), 0)).astype(jnp.float32)
    polar = jnp.pi * (pol_index + 0.5) / (n_th * ct)
    polar_weight = jnp.sqrt(jnp.sin(polar))
    chosen = cells[...].T
    for i in range(cr):
        radius = 1.0 + 2.0 * ((row * cr + i).astype(jnp.float32) + 0.5) / (n_row * cr)
        weighted[i] = jnp.where(lane == chosen[:, i : i + 1], polar_weight * radius, 0.0)

    def rates(stage, i, c_values):
        damped = damping_rate * excision[i].astype(jnp.float32)
        for slot in range(4):
            for s in range(2):
                low = polar_in[stage][0, slot, s, pl.ds(i, 1), :]
                high = polar_in[stage][1, slot, s, pl.ds(i, 1), :]
                padded[stage][slot, i + 2, 6 + s : 7 + s, :] = jnp.where(th > 0, low, 0.0)
                padded[stage][slot, i + 2, 24 + s : 25 + s, :] = jnp.where(th < n_th - 1, high, 0.0)

        def rad(c):
            get = lambda o: padded[stage][SLOT[c], i + 2 + o, 8:24, :]
            return diff(get(1), get(-1), get(2), get(-2), 1.0)

        def pol(c):
            get = lambda o: padded[stage][SLOT[c], i + 2, 8 + o : 24 + o, :]
            return diff(get(1), get(-1), get(2), get(-2), 1.0)

        def azi(c):
            here = padded[stage][SLOT[c], i + 2, 8:24, :]
            edge = outside[EDGE[c], i]
            far_low = pltpu.roll(jnp.where(lane >= cp - 2, edge, here), 2, 1)
            near_low = pltpu.roll(jnp.where(lane >= cp - 1, edge, here), 1, 1)
            near_high = pltpu.roll(jnp.where(lane < 1, edge, here), cp - 1, 1)
            far_high = pltpu.roll(jnp.where(lane < 2, edge, here), cp - 2, 1)
            return diff(near_high, near_low, far_high, far_low, azimuth_gain)

        out = []
        for start, sign in ((3, 1.0), (0, -1.0)):
            curls = (pol(start + 2) - azi(start + 1), azi(start) - rad(start + 2), rad(start + 1) - pol(start))
            for k in range(3):
                c = len(out)
                out.append((curls[k] if sign > 0 else -curls[k]) - damped * c_values[c])
        return out

    def zero_ends(stage):
        low = padded[stage][2:6, 0:2, 8:24, :]
        padded[stage][2:6, 0:2, 8:24, :] = jnp.where(row > 0, low, 0.0)
        high = padded[stage][2:6, 18:20, 8:24, :]
        padded[stage][2:6, 18:20, 8:24, :] = jnp.where(row < n_row - 1, high, 0.0)

    def first_step(i, nothing):
        values = [field[c, i] for c in range(6)]
        rate = rates(0, i, values)
        gain, pick = lapse[i], weighted[i]
        for c in range(6):
            value = values[c] + time_step * rate[c]
            section[c, i] = value
            masked[0][c, at(i), :] = value * pick
            keep_product(1, c, i, gain * value)
        return nothing

    def second_step(i, nothing):
        values = [section[c, i] for c in range(6)]
        rate = rates(1, i, values)
        pick = weighted[i]
        for c in range(6):
            value = 0.5 * (field[c, i] + values[c] + time_step * rate[c])
            fresh[c, i] = value
            masked[1][c, at(i), :] = value * pick
        return nothing

    landed(first_pair, 0)
    first_sum[...] = first_part[...] + first_pair[...]
    for d in range(1, half):
        send(first_sum.at[lax.rem(spot + d, half)], first_plane.at[d - 1], in_half(d), 2)
    remaining = nt(mat[128:256], mat[...])
    other_part[0] = remaining[:, :128].reshape(tiles)
    other_part[1] = remaining[:, 128:].reshape(tiles)
    send(other_part.at[other], other_pair, {"row": y * 2 + other}, 1)
    for copy in halos[0][4:]:
        copy.wait_recv()
    beyond(0)
    landed(other_pair, 1)
    other_sum[...] = other_part[core] + other_pair[...]
    for d in range(1, half):
        send(other_sum.at[lax.rem(spot + d, half)], other_plane.at[d - 1], in_half(d), 3)
    for copy in halos[0][:4]:
        copy.wait_recv()
    zero_ends(0)
    unrolled(first_step, 0)
    for copy in halos[1][:4]:
        copy.start()
    keep_edges(1)
    for copy in halos[1][4:]:
        copy.start()
    sample(0)

    landed(first_plane, 2)
    total = first_sum[spot]
    for d in range(1, half):
        total = total + first_plane[d - 1]
    first_deep[0] = total
    for d in range(1, n_th):
        send(first_deep.at[0], first_deep.at[d], along(d), 4)
    landed(other_plane, 3)
    total = other_sum[spot]
    for d in range(1, half):
        total = total + other_plane[d - 1]
    other_deep[0] = total
    for d in range(1, n_th):
        send(other_deep.at[0], other_deep.at[d], along(d), 5)

    for copy in halos[1][4:]:
        copy.wait_recv()
    beyond(1)
    for copy in halos[1][:4]:
        copy.wait_recv()
    zero_ends(1)
    unrolled(second_step, 0)
    landed(first_deep.at[1:], 4)
    total = first_deep[th]
    for a in range(1, n_th):
        total = total + first_deep[lax.rem(th - a + n_th, n_th)]
    first_full[spot] = total
    for d in range(1, half):
        send(first_full.at[spot], first_full.at[spot], in_half(d), 6)
    sample(1)
    place_row = lax.broadcasted_iota(jnp.int32, (8, mat.shape[1]), 0)
    snap = jnp.where(place_row >= 4, mat[248:256], 0.0)
    cross_plane[0] = nt(snap, mat[...])[4:8]
    for d in range(1, chunks):
        send(cross_plane.at[0], cross_plane.at[d], in_plane(d), 9)
    stores = [pltpu.make_async_copy(fresh, new_ref, store_sem.at[0])]
    stores[0].start()
    square = lax.broadcasted_iota(jnp.int32, (128, 128), 0)
    column = lax.broadcasted_iota(jnp.int32, (128, 128), 1)
    unit = (square == column).astype(jnp.float32)
    work[:, 128:] = unit
    factor[128:256, 0:128] = jnp.zeros((128, 128), jnp.float32)
    padded_low[...] = jnp.zeros_like(padded_low)
    landed(other_deep.at[1:], 5)
    total = other_deep[th]
    for a in range(1, n_th):
        total = total + other_deep[lax.rem(th - a + n_th, n_th)]
    other_full[owner] = total
    for d in range(1, chunks):
        send(other_full.at[owner], other_full.at[owner], in_plane(d), 7)

    landed(first_plane, 6)
    work[:, :128] = first_full[...].reshape(128, 128)
    leaf(work, upper, inverse)
    landed(other_full.at[1:], 7)
    first = inverse[...]
    factor[0:128, 0:128] = upper[...] * (1.0 / scale)
    corner = nt(first, other_full[0:half].reshape(128, 128))
    last = (square >= 124) | (column >= 124)
    work[:, :128] = jnp.where(last, unit, other_full[half:chunks].reshape(128, 128) - tn(corner, corner))
    work[:, 128:] = unit
    landed(cross_plane.at[1:], 9)
    total = cross_plane[owner]
    for a in range(1, chunks):
        total = total + cross_plane[lax.rem(owner - a + chunks, chunks)]
    cross_deep[0] = total
    for d in range(1, n_th):
        send(cross_deep.at[0], cross_deep.at[d], along(d), 10)
    left(first_pair, 0)
    left(other_pair, 1)
    left(first_plane, 2)
    left(other_plane, 3)
    beside = tn(corner, first)
    basis[0:128] = nn(first, mat[0:128]) * scale
    leaf(work, upper, inverse)
    landed(cross_deep.at[1:], 10)
    stores.append(pltpu.make_async_copy(basis.at[0:128], basis_ref.at[0:128], store_sem.at[1]))
    stores[1].start()
    second = inverse[...]
    below = -nn(second, beside)
    cross = cross_deep[th]
    for a in range(1, n_th):
        cross = cross + cross_deep[lax.rem(th - a + n_th, n_th)]
    cross = jnp.concatenate([jnp.zeros((4, 256), jnp.float32), cross], axis=0)
    cross_left, cross_right = cross[:, :128], cross[:, 128:]
    lane8 = lax.broadcasted_iota(jnp.int32, (8, 128), 1)
    sub8 = lax.broadcasted_iota(jnp.int32, (8, 128), 0)
    inner = jnp.where(lane8 < 124, cross_right, 0.0)
    low_left = nt(cross_left, first)
    low_right = jnp.where(lane8 < 124, nt(cross_left, below) + nt(inner, second), 0.0)
    padded_low[120:128, 0:128] = low_left
    padded_low[120:128, 128:256] = low_right
    low = jnp.concatenate([low_left, low_right], axis=1)
    basis[128:256] = (nn(below, mat[0:128]) + nn(second, mat[128:256])) * scale
    snapshot_block = cross_right - nt(low, padded_low[...])
    real = sub8 >= 4
    diagonal = (lane8 == sub8 + 120).astype(jnp.float32)
    snapshot_block = jnp.where(real & (lane8 >= 124), snapshot_block, diagonal)
    rest = snap * scale - nn(low, basis[...])
    _, _, _, solved = eliminate(spread(snapshot_block, 120), jnp.concatenate([snapshot_block, rest], axis=1))
    basis[248:256] = jnp.where(place_row >= 4, solved[:, 128:], basis[248:256])
    stores.append(pltpu.make_async_copy(basis.at[128:256], basis_ref.at[128:256], store_sem.at[2]))
    stores[2].start()
    turned = padded_low[...].T
    factor[0:128, 128:256] = jnp.where(column >= 124, turned[0:128], corner) * (1.0 / scale)
    factor[128:256, 128:256] = jnp.where(column >= 124, turned[128:256], upper[...]) * (1.0 / scale)
    finish = jnp.where(lane8 >= sub8 + 120, solved[:, :128] * (1.0 / scale), 0.0)
    factor[248:256, 128:256] = jnp.where(real, finish, factor[248:256, 128:256])
    stores.append(pltpu.make_async_copy(factor, factor_ref, store_sem.at[3]))
    stores[3].start()

    for stage in range(2):
        for copy in halos[stage]:
            copy.wait_send()
    left(first_deep.at[1:], 4)
    left(other_deep.at[1:], 5)
    left(first_plane, 6)
    left(other_full.at[1:], 7)
    left(cross_plane.at[1:], 9)
    left(cross_deep.at[1:], 10)
    for store in stores:
        store.wait()


def hand_on_kernel(*refs):
    count = (len(refs) - 2) // 3
    sources, targets, held = refs[:count], refs[count : 2 * count], refs[2 * count : 3 * count]
    load_sem, store_sem = refs[3 * count :]
    loads, stores = [], []
    for source, target, through in zip(sources, targets, held):
        pieces = source.shape[0] // 128 if len(source.shape) == 2 else source.shape[0] // 2
        rows = source.shape[0] // pieces
        for k in range(pieces):
            part, n = pl.ds(k * rows, rows), len(loads)
            loads.append(pltpu.make_async_copy(source.at[part], through.at[part], load_sem.at[n]))
            stores.append(pltpu.make_async_copy(through.at[part], target.at[part], store_sem.at[n]))
    for load in loads:
        load.start()
    for load, store in zip(loads, stores):
        load.wait()
        store.start()
    for store in stores:
        store.wait()


def on_device(sizes, fields, lapse_field, excision, sample_cells, old_basis):
    n_row, n_th, n_ph = sizes
    cr, ct, cp = lapse_field.shape
    columns = old_basis.shape[1]
    f32 = jnp.float32
    half = n_row * n_ph // 2
    rows = 128 // half
    cells = sample_cells.reshape(cr, ct)
    vmem = pltpu.VMEM
    scale = math.sqrt(columns * n_row * n_th * n_ph)
    outputs = (
        jax.ShapeDtypeStruct(fields.shape, f32),
        jax.ShapeDtypeStruct((256, columns), f32),
        jax.ShapeDtypeStruct((256, 256), f32),
    )
    results = pl.pallas_call(
        functools.partial(comm_kernel, sizes, scale),
        out_shape=outputs,
        in_specs=[HBM] * 5,
        out_specs=(HBM,) * 3,
        scratch_shapes=[
            vmem(fields.shape, f32),
            vmem(lapse_field.shape, f32),
            vmem(excision.shape, jnp.int32),
            vmem(cells.shape, jnp.int32),
            vmem(old_basis.shape, f32),
            vmem((256, columns), f32),
            vmem(fields.shape, f32),
            vmem(fields.shape, f32),
            vmem(lapse_field.shape, f32),
            vmem((6, cr * ct, cp), f32),
            vmem((6, cr * ct, cp), f32),
            vmem((6, cr + 4, 32, cp), f32),
            vmem((6, cr + 4, 32, cp), f32),
            vmem((2, 4, 2, cr, cp), f32),
            vmem((2, 4, 2, cr, cp), f32),
            vmem((2, 4, 2, cr, cp), f32),
            vmem((2, 4, 2, cr, cp), f32),
            vmem((2, ct, cp), f32),
            vmem((2, ct, cp), f32),
            vmem((2, ct, cp), f32),
            vmem((2, ct, cp), f32),
            vmem((4, cr, ct, cp), f32),
            vmem((half, rows, 128), f32),
            vmem((half, rows, 128), f32),
            vmem((half, rows, 128), f32),
            vmem((half - 1, rows, 128), f32),
            vmem((n_th, rows, 128), f32),
            vmem((half, rows, 128), f32),
            vmem((2, half, rows, 128), f32),
            vmem((half, rows, 128), f32),
            vmem((half, rows, 128), f32),
            vmem((half - 1, rows, 128), f32),
            vmem((n_th, rows, 128), f32),
            vmem((2 * half, rows, 128), f32),
            vmem((2 * half, 4, 256), f32),
            vmem((n_th, 4, 256), f32),
            vmem((128, 256), f32),
            vmem((128, 128), f32),
            vmem((128, 128), f32),
            vmem((128, 256), f32),
            vmem((256, columns), f32),
            vmem((256, 256), f32),
            pltpu.SemaphoreType.DMA((5,)),
            pltpu.SemaphoreType.DMA((4,)),
            pltpu.SemaphoreType.DMA((2, 6)),
            pltpu.SemaphoreType.DMA((2, 6)),
            pltpu.SemaphoreType.DMA((11,)),
            pltpu.SemaphoreType.DMA((11,)),
        ],
        compiler_params=pltpu.CompilerParams(
            collective_id=0, has_side_effects=True, vmem_limit_bytes=LIMIT
        ),
        name="halo_and_gram",
    )(fields, lapse_field, excision, cells, old_basis)
    return pl.pallas_call(
        hand_on_kernel,
        out_shape=outputs,
        in_specs=[HBM] * 3,
        out_specs=(HBM,) * 3,
        scratch_shapes=[vmem(output.shape, f32) for output in outputs]
        + [pltpu.SemaphoreType.DMA((7,)), pltpu.SemaphoreType.DMA((7,))],
        compiler_params=pltpu.CompilerParams(vmem_limit_bytes=LIMIT),
        name="hand_on",
    )(*results)


def solution(mesh):
    sizes = tuple(mesh.shape[name] for name in ("row", "th", "ph"))
    return jax.shard_map(
        functools.partial(on_device, sizes),
        mesh=mesh,
        in_specs=(
            P(None, "row", "th", "ph"),
            P("row", "th", "ph"),
            P("row", "th", "ph"),
            P("row", "th", "ph"),
            P(None, ("row", "th", "ph")),
        ),
        out_specs=(P(None, "row", "th", "ph"), P(None, ("row", "th", "ph")), P()),
        check_vma=False,
    )
```

```python
import functools
import math

import jax
import jax.numpy as jnp
from jax import lax
from jax.experimental import pallas as pl
from jax.experimental.pallas import tpu as pltpu
from jax.sharding import PartitionSpec as P

MESH = pl.DeviceIdType.MESH
LIMIT = 63 * 1024 * 1024
UNROLL = 2
MIDWAY = 10
HIGH = lax.Precision.HIGHEST
HBM = pl.BlockSpec(memory_space=pltpu.HBM)

damping_rate = 3.0
time_step = 0.3
azimuth_gain = 5.0

SLOT = {0: 0, 3: 1, 2: 2, 5: 3, 1: 4, 4: 5}
EDGE = {0: 0, 3: 1, 1: 2, 4: 3}


def nt(a, b):
    return lax.dot_general(a, b, (((1,), (1,)), ((), ())), precision=HIGH, preferred_element_type=jnp.float32)


def nn(a, b):
    return lax.dot_general(a, b, (((1,), (0,)), ((), ())), precision=HIGH, preferred_element_type=jnp.float32)


def tn(a, b):
    return lax.dot_general(a, b, (((0,), (0,)), ((), ())), precision=HIGH, preferred_element_type=jnp.float32)


def diff(near_high, near_low, far_high, far_low, gain):
    return (8.0 * (near_high - near_low) - (far_high - far_low)) * (gain / 12.0)


def sublane(x, k):
    return jnp.broadcast_to(x[k : k + 1], x.shape)


def eliminate(columns, x, follower=None):
    sub = lax.broadcasted_iota(jnp.int32, x.shape, 0)
    columns = list(columns)
    lows, recips, rows = [], [], []
    solved = jnp.zeros_like(x)
    for k in range(8):
        recip = lax.rsqrt(sublane(columns[k], k))
        low = columns[k] * recip
        for b in range(k + 1, 8):
            columns[b] = columns[b] - low * sublane(low, b)
        wide = jnp.tile(recip, (1, x.shape[1] // 128))
        line = sublane(x, k) * wide
        x = x - jnp.tile(low, (1, x.shape[1] // 128)) * line
        solved = jnp.where(sub == k, line, solved)
        lows.append(low)
        recips.append(recip)
        rows.append(line)
        if follower is not None:
            follower(k, recip, low, line)
    return lows, recips, rows, solved


def spread(tile, first):
    return [jnp.broadcast_to(tile[:, first + b : first + b + 1], (8, 128)) for b in range(8)]


def twice(x):
    return jnp.concatenate([x, x], axis=1)


def leaf(work, upper, inverse, midway=None):
    lane = lax.broadcasted_iota(jnp.int32, (8, 128), 1)
    sub = lax.broadcasted_iota(jnp.int32, (8, 128), 0)
    tiles = {t: work[8 * t : 8 * t + 8] for t in range(2)}
    columns = spread(tiles[0], 0)
    for p in range(16):
        if p == MIDWAY and midway is not None:
            midway()
        r0 = 8 * p
        if p < 14:
            tiles[p + 2] = work[r0 + 16 : r0 + 24]
        near = spread(tiles[p + 1], r0) if p < 15 else None
        ahead = spread(tiles[p + 1], r0 + 8) if p < 15 else None
        far = spread(tiles[p + 2], r0) if p < 14 else None

        def follower(k, recip, low, line):
            for t, column in ((p + 1, near), (p + 2, far)):
                if column is None:
                    continue
                mine = column[k] * recip
                tiles[t] = tiles[t] - twice(mine) * line
                for b in range(k + 1, 8):
                    column[b] = column[b] - mine * sublane(low, b)
                if t == p + 1:
                    for b in range(8):
                        ahead[b] = ahead[b] - mine * sublane(mine, b)

        lows, recips, rows, solved = eliminate(columns, tiles[p], follower)
        upper[r0 : r0 + 8] = jnp.where(lane >= sub + r0, solved[:, :128], 0.0)
        inverse[r0 : r0 + 8] = solved[:, 128:]
        columns = ahead
        if p < 13:
            back = [None] * 8
            for q in range(7, -1, -1):
                value = rows[q]
                for a in range(q + 1, 8):
                    value = value - twice(sublane(lows[q], a)) * back[a]
                back[q] = value * twice(recips[q])
            for t in range(p + 3, 16):
                tile = work[8 * t : 8 * t + 8]
                for k, column in enumerate(spread(tile, r0)):
                    tile = tile - twice(column) * back[k]
                work[8 * t : 8 * t + 8] = tile


def comm_kernel(
    sizes, scale,
    fields_ref, lapse_ref, excision_ref, cells_ref, old_ref,
    new_ref, basis_ref, factor_ref,
    field, lapse, excision, cells, old, mat, fresh, section, weighted, masked0, masked1,
    padded0, padded1, polar_out0, polar_out1, polar_in0, polar_in1, edge_out0, edge_out1, edge_in0, edge_in1, outside,
    first_part, first_pair, first_sum, first_plane, first_deep, first_full,
    other_part, other_pair, other_sum, other_plane, other_deep, other_full,
    cross_plane, cross_deep,
    work, upper, inverse, padded_low, basis, factor,
    load_sem, store_sem, halo_send, halo_recv, send_sem, recv_sem,
):
    masked, padded = (masked0, masked1), (padded0, padded1)
    polar_out, polar_in = (polar_out0, polar_out1), (polar_in0, polar_in1)
    edge_out, edge_in = (edge_out0, edge_out1), (edge_in0, edge_in1)
    n_row, n_th, n_ph = sizes
    n_y = n_row // 2
    row, th, ph = lax.axis_index("row"), lax.axis_index("th"), lax.axis_index("ph")
    core, y = lax.rem(row, 2), lax.div(row, 2)
    spot = y * n_ph + ph
    half = n_y * n_ph
    chunks = 2 * half
    owner = core * half + spot
    cr, ct, cp = 16, 16, 128

    loads = [
        pltpu.make_async_copy(source, target, load_sem.at[k])
        for k, (source, target) in enumerate(
            (
                (old_ref.at[0:128], old.at[0:128]),
                (fields_ref, field),
                (lapse_ref, lapse),
                (excision_ref, excision),
                (cells_ref, cells),
                (old_ref.at[128:252], old.at[128:252]),
            )
        )
    ]
    for load in loads:
        load.start()

    def place(index):
        which, rest = lax.div(index, half), lax.rem(index, half)
        return {"row": lax.div(rest, n_ph) * 2 + which, "ph": lax.rem(rest, n_ph)}

    def in_plane(d):
        return place(lax.rem(owner + d, chunks))

    def in_half(d):
        return place(core * half + lax.rem(spot + d, half))

    def along(d):
        return {"th": lax.rem(th + d, n_th)}

    barrier = pltpu.get_barrier_semaphore()
    for d in range(1, chunks):
        pl.semaphore_signal(barrier, inc=1, device_id=in_plane(d), device_id_type=MESH)
    for d in range(1, n_th):
        pl.semaphore_signal(barrier, inc=1, device_id=along(d), device_id_type=MESH)

    def send(source, target, device, k):
        copy = pltpu.make_async_remote_copy(
            src_ref=source, dst_ref=target, send_sem=send_sem.at[k], recv_sem=recv_sem.at[k],
            device_id=device, device_id_type=MESH,
        )
        copy.start()

    def landed(ref, k):
        pltpu.make_async_copy(ref, ref, recv_sem.at[k]).wait()

    def left(ref, k):
        pltpu.make_async_copy(ref, ref, send_sem.at[k]).wait()

    lane = lax.broadcasted_iota(jnp.int32, (ct, cp), 1)
    lane_pair = lax.shift_right_logical(lane, 1)

    loads[0].wait()
    tiles = first_part.shape
    first_part[...] = nt(old[0:128], old[0:128]).reshape(tiles)
    pl.semaphore_wait(barrier, chunks - 1 + n_th - 1)
    other = 1 - core
    send(first_part, first_pair, {"row": y * 2 + other}, 0)

    def keep_product(stage, c, i, value):
        slot = SLOT[c]
        padded[stage][slot, i + 2, 8:24, :] = value
        if slot < 4:
            for s in range(2):
                polar_out[stage][0, slot, s, pl.ds(i, 1), :] = value[s : s + 1]
                polar_out[stage][1, slot, s, pl.ds(i, 1), :] = value[14 + s : 15 + s]

    def keep_edges(stage):
        low = high = jnp.zeros((ct, cp), jnp.float32)
        for c, e in EDGE.items():
            for i in range(cr):
                t = e * cr + i
                value = padded[stage][SLOT[c], i + 2, 8:24, :]
                here = lane_pair == t
                low = jnp.where(here, pltpu.roll(value, 2 * t, 1), low)
                high = jnp.where(here, pltpu.roll(value, (2 * t + 2) % cp, 1), high)
        edge_out[stage][0] = low
        edge_out[stage][1] = high

    def beyond(stage):
        low, high = edge_in[stage][0], edge_in[stage][1]
        for e in range(4):
            for i in range(cr):
                t = e * cr + i
                moved = pltpu.roll(high, (cp - 2 * t) % cp, 1), pltpu.roll(low, cp - 2 - 2 * t, 1)
                outside[e, i] = jnp.where(lane < cp // 2, *moved)

    def unrolled(body, carry, by=UNROLL):
        def several(k, carry):
            for u in range(by):
                carry = body(k * by + u, carry)
            return carry

        if by == cr:
            return several(0, carry)
        return lax.fori_loop(0, cr // by, several, carry)

    def sample(stage):
        for c in range(6):
            for h in range(cr * ct // cp):
                line = jnp.sum(masked[stage][c, h * cp : (h + 1) * cp, :].T, axis=0, keepdims=True)
                r, first = 252 + 2 * stage + c // 3, (c % 3) * cr * ct + h * cp
                mat[r : r + 1, first : first + cp] = line

    def at(i):
        return slice(i * ct, (i + 1) * ct) if isinstance(i, int) else pl.ds(pl.multiple_of(i * ct, ct), ct)

    def first_products(i, nothing):
        gain = lapse[i]
        for c in range(6):
            keep_product(0, c, i, gain * field[c, i])
        return nothing

    def halo_copies(stage):
        rows = ((padded[stage].at[2:6, 2:4, 8:24, :], padded[stage].at[2:6, 18:20, 8:24, :], {"row": lax.rem(row + n_row - 1, n_row)}),
                (padded[stage].at[2:6, 16:18, 8:24, :], padded[stage].at[2:6, 0:2, 8:24, :], {"row": lax.rem(row + 1, n_row)}))
        polars = ((polar_out[stage].at[0], polar_in[stage].at[1], {"th": lax.rem(th + n_th - 1, n_th)}),
                  (polar_out[stage].at[1], polar_in[stage].at[0], {"th": lax.rem(th + 1, n_th)}))
        edges = ((edge_out[stage].at[0], edge_in[stage].at[1], {"ph": lax.rem(ph + n_ph - 1, n_ph)}),
                 (edge_out[stage].at[1], edge_in[stage].at[0], {"ph": lax.rem(ph + 1, n_ph)}))
        return [
            pltpu.make_async_remote_copy(
                src_ref=source, dst_ref=target, send_sem=halo_send.at[stage, k], recv_sem=halo_recv.at[stage, k],
                device_id=device, device_id_type=MESH,
            )
            for k, (source, target, device) in enumerate(rows + polars + edges)
        ]

    for load in loads[1:]:
        load.wait()
    unrolled(first_products, 0, cr)
    keep_edges(0)

    halos = [halo_copies(0), halo_copies(1)]
    for copy in halos[0]:
        copy.start()
    pol_index = (th * ct + lax.broadcasted_iota(jnp.int32, (ct, cp), 0)).astype(jnp.float32)
    polar = jnp.pi * (pol_index + 0.5) / (n_th * ct)
    polar_weight = jnp.sqrt(jnp.sin(polar))
    chosen = cells[...].T
    for i in range(cr):
        radius = 1.0 + 2.0 * ((row * cr + i).astype(jnp.float32) + 0.5) / (n_row * cr)
        weighted[i] = jnp.where(lane == chosen[:, i : i + 1], polar_weight * radius, 0.0)

    def rates(stage, i, c_values):
        damped = damping_rate * excision[i].astype(jnp.float32)
        for slot in range(4):
            for s in range(2):
                low = polar_in[stage][0, slot, s, pl.ds(i, 1), :]
                high = polar_in[stage][1, slot, s, pl.ds(i, 1), :]
                padded[stage][slot, i + 2, 6 + s : 7 + s, :] = jnp.where(th > 0, low, 0.0)
                padded[stage][slot, i + 2, 24 + s : 25 + s, :] = jnp.where(th < n_th - 1, high, 0.0)

        def rad(c):
            get = lambda o: padded[stage][SLOT[c], i + 2 + o, 8:24, :]
            return diff(get(1), get(-1), get(2), get(-2), 1.0)

        def pol(c):
            get = lambda o: padded[stage][SLOT[c], i + 2, 8 + o : 24 + o, :]
            return diff(get(1), get(-1), get(2), get(-2), 1.0)

        def azi(c):
            here = padded[stage][SLOT[c], i + 2, 8:24, :]
            edge = outside[EDGE[c], i]
            far_low = pltpu.roll(jnp.where(lane >= cp - 2, edge, here), 2, 1)
            near_low = pltpu.roll(jnp.where(lane >= cp - 1, edge, here), 1, 1)
            near_high = pltpu.roll(jnp.where(lane < 1, edge, here), cp - 1, 1)
            far_high = pltpu.roll(jnp.where(lane < 2, edge, here), cp - 2, 1)
            return diff(near_high, near_low, far_high, far_low, azimuth_gain)

        out = []
        for start, sign in ((3, 1.0), (0, -1.0)):
            curls = (pol(start + 2) - azi(start + 1), azi(start) - rad(start + 2), rad(start + 1) - pol(start))
            for k in range(3):
                c = len(out)
                out.append((curls[k] if sign > 0 else -curls[k]) - damped * c_values[c])
        return out

    def zero_ends(stage):
        low = padded[stage][2:6, 0:2, 8:24, :]
        padded[stage][2:6, 0:2, 8:24, :] = jnp.where(row > 0, low, 0.0)
        high = padded[stage][2:6, 18:20, 8:24, :]
        padded[stage][2:6, 18:20, 8:24, :] = jnp.where(row < n_row - 1, high, 0.0)

    def first_step(i, nothing):
        values = [field[c, i] for c in range(6)]
        rate = rates(0, i, values)
        gain, pick = lapse[i], weighted[i]
        for c in range(6):
            value = values[c] + time_step * rate[c]
            section[c, i] = value
            masked[0][c, at(i), :] = value * pick
            keep_product(1, c, i, gain * value)
        return nothing

    def second_step(i, nothing):
        values = [section[c, i] for c in range(6)]
        rate = rates(1, i, values)
        pick = weighted[i]
        for c in range(6):
            value = 0.5 * (field[c, i] + values[c] + time_step * rate[c])
            fresh[c, i] = value
            masked[1][c, at(i), :] = value * pick
        return nothing

    landed(first_pair, 0)
    first_sum[...] = first_part[...] + first_pair[...]
    for d in range(1, half):
        send(first_sum.at[lax.rem(spot + d, half)], first_plane.at[d - 1], in_half(d), 2)
    mat[0:248] = old[0:248]
    mat[248:252] = old[248:252]
    mat[252:256] = jnp.zeros((4, mat.shape[1]), jnp.float32)
    remaining = nt(mat[128:256], mat[...])
    other_part[0] = remaining[:, :128].reshape(tiles)
    other_part[1] = remaining[:, 128:].reshape(tiles)
    send(other_part.at[other], other_pair, {"row": y * 2 + other}, 1)
    for copy in halos[0][4:]:
        copy.wait_recv()
    beyond(0)
    landed(other_pair, 1)
    other_sum[...] = other_part[core] + other_pair[...]
    for d in range(1, half):
        send(other_sum.at[lax.rem(spot + d, half)], other_plane.at[d - 1], in_half(d), 3)
    for copy in halos[0][:4]:
        copy.wait_recv()
    zero_ends(0)
    unrolled(first_step, 0)
    for copy in halos[1][:4]:
        copy.start()
    keep_edges(1)
    for copy in halos[1][4:]:
        copy.start()
    sample(0)

    landed(first_plane, 2)
    total = first_sum[spot]
    for d in range(1, half):
        total = total + first_plane[d - 1]
    first_deep[0] = total
    for d in range(1, n_th):
        send(first_deep.at[0], first_deep.at[d], along(d), 4)
    landed(other_plane, 3)
    total = other_sum[spot]
    for d in range(1, half):
        total = total + other_plane[d - 1]
    other_deep[0] = total
    for d in range(1, n_th):
        send(other_deep.at[0], other_deep.at[d], along(d), 5)

    for copy in halos[1][4:]:
        copy.wait_recv()
    beyond(1)
    for copy in halos[1][:4]:
        copy.wait_recv()
    zero_ends(1)
    unrolled(second_step, 0)
    sample(1)
    landed(first_deep.at[1:], 4)
    total = first_deep[th]
    for a in range(1, n_th):
        total = total + first_deep[lax.rem(th - a + n_th, n_th)]
    first_full[spot] = total
    for d in range(1, half):
        send(first_full.at[spot], first_full.at[spot], in_half(d), 6)
    place_row = lax.broadcasted_iota(jnp.int32, (8, mat.shape[1]), 0)
    snap = jnp.where(place_row >= 4, mat[248:256], 0.0)
    cross_plane[0] = nt(snap, mat[...])[4:8]
    for d in range(1, chunks):
        send(cross_plane.at[0], cross_plane.at[d], in_plane(d), 9)
    stores = [pltpu.make_async_copy(fresh, new_ref, store_sem.at[0])]
    stores[0].start()
    square = lax.broadcasted_iota(jnp.int32, (128, 128), 0)
    column = lax.broadcasted_iota(jnp.int32, (128, 128), 1)
    unit = (square == column).astype(jnp.float32)
    work[:, 128:] = unit
    factor[128:256, 0:128] = jnp.zeros((128, 128), jnp.float32)
    padded_low[...] = jnp.zeros_like(padded_low)
    landed(other_deep.at[1:], 5)
    total = other_deep[th]
    for a in range(1, n_th):
        total = total + other_deep[lax.rem(th - a + n_th, n_th)]
    other_full[owner] = total
    for d in range(1, chunks):
        send(other_full.at[owner], other_full.at[owner], in_plane(d), 7)

    landed(first_plane, 6)
    work[:, :128] = first_full[...].reshape(128, 128)
    def sum_cross():
        landed(cross_plane.at[1:], 9)
        total = cross_plane[owner]
        for a in range(1, chunks):
            total = total + cross_plane[lax.rem(owner - a + chunks, chunks)]
        cross_deep[0] = total
        for d in range(1, n_th):
            send(cross_deep.at[0], cross_deep.at[d], along(d), 10)
        left(first_pair, 0)
        left(other_pair, 1)
        left(first_plane, 2)
        left(other_plane, 3)

    leaf(work, upper, inverse, sum_cross)
    landed(other_full.at[1:], 7)
    first = inverse[...]
    factor[0:128, 0:128] = upper[...] * (1.0 / scale)
    corner = nt(first, other_full[0:half].reshape(128, 128))
    last = (square >= 124) | (column >= 124)
    work[:, :128] = jnp.where(last, unit, other_full[half:chunks].reshape(128, 128) - tn(corner, corner))
    work[:, 128:] = unit
    beside = tn(corner, first)
    basis[0:128] = nn(first, mat[0:128]) * scale
    leaf(work, upper, inverse)
    landed(cross_deep.at[1:], 10)
    stores.append(pltpu.make_async_copy(basis.at[0:128], basis_ref.at[0:128], store_sem.at[1]))
    stores[1].start()
    second = inverse[...]
    below = -nn(second, beside)
    cross = cross_deep[th]
    for a in range(1, n_th):
        cross = cross + cross_deep[lax.rem(th - a + n_th, n_th)]
    cross = jnp.concatenate([jnp.zeros((4, 256), jnp.float32), cross], axis=0)
    cross_left, cross_right = cross[:, :128], cross[:, 128:]
    lane8 = lax.broadcasted_iota(jnp.int32, (8, 128), 1)
    sub8 = lax.broadcasted_iota(jnp.int32, (8, 128), 0)
    inner = jnp.where(lane8 < 124, cross_right, 0.0)
    low_left = nt(cross_left, first)
    low_right = jnp.where(lane8 < 124, nt(cross_left, below) + nt(inner, second), 0.0)
    padded_low[120:128, 0:128] = low_left
    padded_low[120:128, 128:256] = low_right
    low = jnp.concatenate([low_left, low_right], axis=1)
    basis[128:256] = (nn(below, mat[0:128]) + nn(second, mat[128:256])) * scale
    snapshot_block = cross_right - nt(low, padded_low[...])
    real = sub8 >= 4
    diagonal = (lane8 == sub8 + 120).astype(jnp.float32)
    snapshot_block = jnp.where(real & (lane8 >= 124), snapshot_block, diagonal)
    rest = snap * scale - nn(low, basis[...])
    _, _, _, solved = eliminate(spread(snapshot_block, 120), jnp.concatenate([snapshot_block, rest], axis=1))
    basis[248:256] = jnp.where(place_row >= 4, solved[:, 128:], basis[248:256])
    stores.append(pltpu.make_async_copy(basis.at[128:256], basis_ref.at[128:256], store_sem.at[2]))
    stores[2].start()
    turned = padded_low[...].T
    factor[0:128, 128:256] = jnp.where(column >= 124, turned[0:128], corner) * (1.0 / scale)
    factor[128:256, 128:256] = jnp.where(column >= 124, turned[128:256], upper[...]) * (1.0 / scale)
    finish = jnp.where(lane8 >= sub8 + 120, solved[:, :128] * (1.0 / scale), 0.0)
    factor[248:256, 128:256] = jnp.where(real, finish, factor[248:256, 128:256])
    stores.append(pltpu.make_async_copy(factor, factor_ref, store_sem.at[3]))
    stores[3].start()

    for stage in range(2):
        for copy in halos[stage]:
            copy.wait_send()
    left(first_deep.at[1:], 4)
    left(other_deep.at[1:], 5)
    left(first_plane, 6)
    left(other_full.at[1:], 7)
    left(cross_plane.at[1:], 9)
    left(cross_deep.at[1:], 10)
    for store in stores:
        store.wait()


def hand_on_kernel(*refs):
    count = (len(refs) - 2) // 3
    sources, targets, held = refs[:count], refs[count : 2 * count], refs[2 * count : 3 * count]
    load_sem, store_sem = refs[3 * count :]
    loads, stores = [], []
    for source, target, through in zip(sources, targets, held):
        pieces = source.shape[0] // 128 if len(source.shape) == 2 else source.shape[0] // 2
        rows = source.shape[0] // pieces
        for k in range(pieces):
            part, n = pl.ds(k * rows, rows), len(loads)
            loads.append(pltpu.make_async_copy(source.at[part], through.at[part], load_sem.at[n]))
            stores.append(pltpu.make_async_copy(through.at[part], target.at[part], store_sem.at[n]))
    for load in loads:
        load.start()
    for load, store in zip(loads, stores):
        load.wait()
        store.start()
    for store in stores:
        store.wait()


def on_device(sizes, fields, lapse_field, excision, sample_cells, old_basis):
    n_row, n_th, n_ph = sizes
    cr, ct, cp = lapse_field.shape
    columns = old_basis.shape[1]
    f32 = jnp.float32
    half = n_row * n_ph // 2
    rows = 128 // half
    cells = sample_cells.reshape(cr, ct)
    vmem = pltpu.VMEM
    scale = math.sqrt(columns * n_row * n_th * n_ph)
    outputs = (
        jax.ShapeDtypeStruct(fields.shape, f32),
        jax.ShapeDtypeStruct((256, columns), f32),
        jax.ShapeDtypeStruct((256, 256), f32),
    )
    results = pl.pallas_call(
        functools.partial(comm_kernel, sizes, scale),
        out_shape=outputs,
        in_specs=[HBM] * 5,
        out_specs=(HBM,) * 3,
        scratch_shapes=[
            vmem(fields.shape, f32),
            vmem(lapse_field.shape, f32),
            vmem(excision.shape, jnp.int32),
            vmem(cells.shape, jnp.int32),
            vmem(old_basis.shape, f32),
            vmem((256, columns), f32),
            vmem(fields.shape, f32),
            vmem(fields.shape, f32),
            vmem(lapse_field.shape, f32),
            vmem((6, cr * ct, cp), f32),
            vmem((6, cr * ct, cp), f32),
            vmem((6, cr + 4, 32, cp), f32),
            vmem((6, cr + 4, 32, cp), f32),
            vmem((2, 4, 2, cr, cp), f32),
            vmem((2, 4, 2, cr, cp), f32),
            vmem((2, 4, 2, cr, cp), f32),
            vmem((2, 4, 2, cr, cp), f32),
            vmem((2, ct, cp), f32),
            vmem((2, ct, cp), f32),
            vmem((2, ct, cp), f32),
            vmem((2, ct, cp), f32),
            vmem((4, cr, ct, cp), f32),
            vmem((half, rows, 128), f32),
            vmem((half, rows, 128), f32),
            vmem((half, rows, 128), f32),
            vmem((half - 1, rows, 128), f32),
            vmem((n_th, rows, 128), f32),
            vmem((half, rows, 128), f32),
            vmem((2, half, rows, 128), f32),
            vmem((half, rows, 128), f32),
            vmem((half, rows, 128), f32),
            vmem((half - 1, rows, 128), f32),
            vmem((n_th, rows, 128), f32),
            vmem((2 * half, rows, 128), f32),
            vmem((2 * half, 4, 256), f32),
            vmem((n_th, 4, 256), f32),
            vmem((128, 256), f32),
            vmem((128, 128), f32),
            vmem((128, 128), f32),
            vmem((128, 256), f32),
            vmem((256, columns), f32),
            vmem((256, 256), f32),
            pltpu.SemaphoreType.DMA((6,)),
            pltpu.SemaphoreType.DMA((4,)),
            pltpu.SemaphoreType.DMA((2, 6)),
            pltpu.SemaphoreType.DMA((2, 6)),
            pltpu.SemaphoreType.DMA((11,)),
            pltpu.SemaphoreType.DMA((11,)),
        ],
        compiler_params=pltpu.CompilerParams(
            collective_id=0, has_side_effects=True, vmem_limit_bytes=LIMIT
        ),
        name="halo_and_gram",
    )(fields, lapse_field, excision, cells, old_basis)
    return pl.pallas_call(
        hand_on_kernel,
        out_shape=outputs,
        in_specs=[HBM] * 3,
        out_specs=(HBM,) * 3,
        scratch_shapes=[vmem(output.shape, f32) for output in outputs]
        + [pltpu.SemaphoreType.DMA((7,)), pltpu.SemaphoreType.DMA((7,))],
        compiler_params=pltpu.CompilerParams(vmem_limit_bytes=LIMIT),
        name="hand_on",
    )(*results)


def solution(mesh):
    sizes = tuple(mesh.shape[name] for name in ("row", "th", "ph"))
    return jax.shard_map(
        functools.partial(on_device, sizes),
        mesh=mesh,
        in_specs=(
            P(None, "row", "th", "ph"),
            P("row", "th", "ph"),
            P("row", "th", "ph"),
            P("row", "th", "ph"),
            P(None, ("row", "th", "ph")),
        ),
        out_specs=(P(None, "row", "th", "ph"), P(None, ("row", "th", "ph")), P()),
        check_vma=False,
    )
```

```python
import functools
import math

import jax
import jax.numpy as jnp
from jax import lax
from jax.experimental import pallas as pl
from jax.experimental.pallas import tpu as pltpu
from jax.sharding import PartitionSpec as P

MESH = pl.DeviceIdType.MESH
LIMIT = 63 * 1024 * 1024
UNROLL = 2
MIDWAY = 10
HIGH = lax.Precision.HIGHEST
HBM = pl.BlockSpec(memory_space=pltpu.HBM)

damping_rate = 3.0
time_step = 0.3
azimuth_gain = 5.0

SLOT = {0: 0, 3: 1, 2: 2, 5: 3, 1: 4, 4: 5}
EDGE = {0: 0, 3: 1, 1: 2, 4: 3}


def nt(a, b):
    return lax.dot_general(a, b, (((1,), (1,)), ((), ())), precision=HIGH, preferred_element_type=jnp.float32)


def nn(a, b):
    return lax.dot_general(a, b, (((1,), (0,)), ((), ())), precision=HIGH, preferred_element_type=jnp.float32)


def tn(a, b):
    return lax.dot_general(a, b, (((0,), (0,)), ((), ())), precision=HIGH, preferred_element_type=jnp.float32)


def diff(near_high, near_low, far_high, far_low, gain):
    return (8.0 * (near_high - near_low) - (far_high - far_low)) * (gain / 12.0)


def sublane(x, k):
    return jnp.broadcast_to(x[k : k + 1], x.shape)


def eliminate(columns, x, follower=None):
    sub = lax.broadcasted_iota(jnp.int32, x.shape, 0)
    columns = list(columns)
    lows, recips, rows = [], [], []
    solved = jnp.zeros_like(x)
    for k in range(8):
        recip = lax.rsqrt(sublane(columns[k], k))
        low = columns[k] * recip
        for b in range(k + 1, 8):
            columns[b] = columns[b] - low * sublane(low, b)
        wide = jnp.tile(recip, (1, x.shape[1] // 128))
        line = sublane(x, k) * wide
        x = x - jnp.tile(low, (1, x.shape[1] // 128)) * line
        solved = jnp.where(sub == k, line, solved)
        lows.append(low)
        recips.append(recip)
        rows.append(line)
        if follower is not None:
            follower(k, recip, low, line)
    return lows, recips, rows, solved


def spread(tile, first):
    return [jnp.broadcast_to(tile[:, first + b : first + b + 1], (8, 128)) for b in range(8)]


def twice(x):
    return jnp.concatenate([x, x], axis=1)


def leaf(work, upper, inverse, midway=None):
    lane = lax.broadcasted_iota(jnp.int32, (8, 128), 1)
    sub = lax.broadcasted_iota(jnp.int32, (8, 128), 0)
    tiles = {t: work[8 * t : 8 * t + 8] for t in range(2)}
    columns = spread(tiles[0], 0)
    for p in range(16):
        if p == MIDWAY and midway is not None:
            midway()
        r0 = 8 * p
        if p < 14:
            tiles[p + 2] = work[r0 + 16 : r0 + 24]
        near = spread(tiles[p + 1], r0) if p < 15 else None
        ahead = spread(tiles[p + 1], r0 + 8) if p < 15 else None
        far = spread(tiles[p + 2], r0) if p < 14 else None

        def follower(k, recip, low, line):
            for t, column in ((p + 1, near), (p + 2, far)):
                if column is None:
                    continue
                mine = column[k] * recip
                tiles[t] = tiles[t] - twice(mine) * line
                for b in range(k + 1, 8):
                    column[b] = column[b] - mine * sublane(low, b)
                if t == p + 1:
                    for b in range(8):
                        ahead[b] = ahead[b] - mine * sublane(mine, b)

        lows, recips, rows, solved = eliminate(columns, tiles[p], follower)
        upper[r0 : r0 + 8] = jnp.where(lane >= sub + r0, solved[:, :128], 0.0)
        inverse[r0 : r0 + 8] = solved[:, 128:]
        columns = ahead
        if p < 13:
            back = [None] * 8
            for q in range(7, -1, -1):
                value = rows[q]
                for a in range(q + 1, 8):
                    value = value - twice(sublane(lows[q], a)) * back[a]
                back[q] = value * twice(recips[q])
            for t in range(p + 3, 16):
                tile = work[8 * t : 8 * t + 8]
                for k, column in enumerate(spread(tile, r0)):
                    tile = tile - twice(column) * back[k]
                work[8 * t : 8 * t + 8] = tile


def comm_kernel(
    sizes, scale,
    fields_ref, lapse_ref, excision_ref, cells_ref, old_ref,
    new_ref, rows_ref, blocks_ref, cross_ref,
    field, lapse, excision, cells, old, mat, fresh, section, weighted, masked0, masked1,
    padded0, padded1, polar_out0, polar_out1, polar_in0, polar_in1, edge_out0, edge_out1, edge_in0, edge_in1, outside,
    first_part, first_pair, first_sum, first_plane, first_deep, first_full,
    other_part, other_pair, other_sum, other_plane, other_deep, other_full,
    cross_plane, cross_deep,
    work, upper, inverse, rows, blocks, cross_sum,
    load_sem, store_sem, halo_send, halo_recv, send_sem, recv_sem,
):
    masked, padded = (masked0, masked1), (padded0, padded1)
    polar_out, polar_in = (polar_out0, polar_out1), (polar_in0, polar_in1)
    edge_out, edge_in = (edge_out0, edge_out1), (edge_in0, edge_in1)
    n_row, n_th, n_ph = sizes
    n_y = n_row // 2
    row, th, ph = lax.axis_index("row"), lax.axis_index("th"), lax.axis_index("ph")
    core, y = lax.rem(row, 2), lax.div(row, 2)
    spot = y * n_ph + ph
    half = n_y * n_ph
    chunks = 2 * half
    owner = core * half + spot
    cr, ct, cp = 16, 16, 128

    loads = [
        pltpu.make_async_copy(source, target, load_sem.at[k])
        for k, (source, target) in enumerate(
            (
                (old_ref.at[0:128], old.at[0:128]),
                (fields_ref, field),
                (lapse_ref, lapse),
                (excision_ref, excision),
                (cells_ref, cells),
                (old_ref.at[128:252], old.at[128:252]),
            )
        )
    ]
    for load in loads:
        load.start()

    def place(index):
        which, rest = lax.div(index, half), lax.rem(index, half)
        return {"row": lax.div(rest, n_ph) * 2 + which, "ph": lax.rem(rest, n_ph)}

    def in_plane(d):
        return place(lax.rem(owner + d, chunks))

    def in_half(d):
        return place(core * half + lax.rem(spot + d, half))

    def along(d):
        return {"th": lax.rem(th + d, n_th)}

    barrier = pltpu.get_barrier_semaphore()
    for d in range(1, chunks):
        pl.semaphore_signal(barrier, inc=1, device_id=in_plane(d), device_id_type=MESH)
    for d in range(1, n_th):
        pl.semaphore_signal(barrier, inc=1, device_id=along(d), device_id_type=MESH)

    def send(source, target, device, k):
        copy = pltpu.make_async_remote_copy(
            src_ref=source, dst_ref=target, send_sem=send_sem.at[k], recv_sem=recv_sem.at[k],
            device_id=device, device_id_type=MESH,
        )
        copy.start()

    def landed(ref, k):
        pltpu.make_async_copy(ref, ref, recv_sem.at[k]).wait()

    def left(ref, k):
        pltpu.make_async_copy(ref, ref, send_sem.at[k]).wait()

    lane = lax.broadcasted_iota(jnp.int32, (ct, cp), 1)
    lane_pair = lax.shift_right_logical(lane, 1)

    loads[0].wait()
    tiles = first_part.shape
    first_part[...] = nt(old[0:128], old[0:128]).reshape(tiles)
    pl.semaphore_wait(barrier, chunks - 1 + n_th - 1)
    other = 1 - core
    send(first_part, first_pair, {"row": y * 2 + other}, 0)

    def keep_product(stage, c, i, value):
        slot = SLOT[c]
        padded[stage][slot, i + 2, 8:24, :] = value
        if slot < 4:
            for s in range(2):
                polar_out[stage][0, slot, s, pl.ds(i, 1), :] = value[s : s + 1]
                polar_out[stage][1, slot, s, pl.ds(i, 1), :] = value[14 + s : 15 + s]

    def keep_edges(stage):
        low = high = jnp.zeros((ct, cp), jnp.float32)
        for c, e in EDGE.items():
            for i in range(cr):
                t = e * cr + i
                value = padded[stage][SLOT[c], i + 2, 8:24, :]
                here = lane_pair == t
                low = jnp.where(here, pltpu.roll(value, 2 * t, 1), low)
                high = jnp.where(here, pltpu.roll(value, (2 * t + 2) % cp, 1), high)
        edge_out[stage][0] = low
        edge_out[stage][1] = high

    def beyond(stage):
        low, high = edge_in[stage][0], edge_in[stage][1]
        for e in range(4):
            for i in range(cr):
                t = e * cr + i
                moved = pltpu.roll(high, (cp - 2 * t) % cp, 1), pltpu.roll(low, cp - 2 - 2 * t, 1)
                outside[e, i] = jnp.where(lane < cp // 2, *moved)

    def unrolled(body, carry, by=UNROLL):
        def several(k, carry):
            for u in range(by):
                carry = body(k * by + u, carry)
            return carry

        if by == cr:
            return several(0, carry)
        return lax.fori_loop(0, cr // by, several, carry)

    def sample(stage):
        for c in range(6):
            for h in range(cr * ct // cp):
                line = jnp.sum(masked[stage][c, h * cp : (h + 1) * cp, :].T, axis=0, keepdims=True)
                r, first = 252 + 2 * stage + c // 3, (c % 3) * cr * ct + h * cp
                mat[r : r + 1, first : first + cp] = line

    def at(i):
        return slice(i * ct, (i + 1) * ct) if isinstance(i, int) else pl.ds(pl.multiple_of(i * ct, ct), ct)

    def first_products(i, nothing):
        gain = lapse[i]
        for c in range(6):
            keep_product(0, c, i, gain * field[c, i])
        return nothing

    def halo_copies(stage):
        rows = ((padded[stage].at[2:6, 2:4, 8:24, :], padded[stage].at[2:6, 18:20, 8:24, :], {"row": lax.rem(row + n_row - 1, n_row)}),
                (padded[stage].at[2:6, 16:18, 8:24, :], padded[stage].at[2:6, 0:2, 8:24, :], {"row": lax.rem(row + 1, n_row)}))
        polars = ((polar_out[stage].at[0], polar_in[stage].at[1], {"th": lax.rem(th + n_th - 1, n_th)}),
                  (polar_out[stage].at[1], polar_in[stage].at[0], {"th": lax.rem(th + 1, n_th)}))
        edges = ((edge_out[stage].at[0], edge_in[stage].at[1], {"ph": lax.rem(ph + n_ph - 1, n_ph)}),
                 (edge_out[stage].at[1], edge_in[stage].at[0], {"ph": lax.rem(ph + 1, n_ph)}))
        return [
            pltpu.make_async_remote_copy(
                src_ref=source, dst_ref=target, send_sem=halo_send.at[stage, k], recv_sem=halo_recv.at[stage, k],
                device_id=device, device_id_type=MESH,
            )
            for k, (source, target, device) in enumerate(rows + polars + edges)
        ]

    for load in loads[1:]:
        load.wait()
    unrolled(first_products, 0, cr)
    keep_edges(0)

    halos = [halo_copies(0), halo_copies(1)]
    for copy in halos[0]:
        copy.start()
    pol_index = (th * ct + lax.broadcasted_iota(jnp.int32, (ct, cp), 0)).astype(jnp.float32)
    polar = jnp.pi * (pol_index + 0.5) / (n_th * ct)
    polar_weight = jnp.sqrt(jnp.sin(polar))
    chosen = cells[...].T
    for i in range(cr):
        radius = 1.0 + 2.0 * ((row * cr + i).astype(jnp.float32) + 0.5) / (n_row * cr)
        weighted[i] = jnp.where(lane == chosen[:, i : i + 1], polar_weight * radius, 0.0)

    def rates(stage, i, c_values):
        damped = damping_rate * excision[i].astype(jnp.float32)
        for slot in range(4):
            for s in range(2):
                low = polar_in[stage][0, slot, s, pl.ds(i, 1), :]
                high = polar_in[stage][1, slot, s, pl.ds(i, 1), :]
                padded[stage][slot, i + 2, 6 + s : 7 + s, :] = jnp.where(th > 0, low, 0.0)
                padded[stage][slot, i + 2, 24 + s : 25 + s, :] = jnp.where(th < n_th - 1, high, 0.0)

        def rad(c):
            get = lambda o: padded[stage][SLOT[c], i + 2 + o, 8:24, :]
            return diff(get(1), get(-1), get(2), get(-2), 1.0)

        def pol(c):
            get = lambda o: padded[stage][SLOT[c], i + 2, 8 + o : 24 + o, :]
            return diff(get(1), get(-1), get(2), get(-2), 1.0)

        def azi(c):
            here = padded[stage][SLOT[c], i + 2, 8:24, :]
            edge = outside[EDGE[c], i]
            far_low = pltpu.roll(jnp.where(lane >= cp - 2, edge, here), 2, 1)
            near_low = pltpu.roll(jnp.where(lane >= cp - 1, edge, here), 1, 1)
            near_high = pltpu.roll(jnp.where(lane < 1, edge, here), cp - 1, 1)
            far_high = pltpu.roll(jnp.where(lane < 2, edge, here), cp - 2, 1)
            return diff(near_high, near_low, far_high, far_low, azimuth_gain)

        out = []
        for start, sign in ((3, 1.0), (0, -1.0)):
            curls = (pol(start + 2) - azi(start + 1), azi(start) - rad(start + 2), rad(start + 1) - pol(start))
            for k in range(3):
                c = len(out)
                out.append((curls[k] if sign > 0 else -curls[k]) - damped * c_values[c])
        return out

    def zero_ends(stage):
        low = padded[stage][2:6, 0:2, 8:24, :]
        padded[stage][2:6, 0:2, 8:24, :] = jnp.where(row > 0, low, 0.0)
        high = padded[stage][2:6, 18:20, 8:24, :]
        padded[stage][2:6, 18:20, 8:24, :] = jnp.where(row < n_row - 1, high, 0.0)

    def first_step(i, nothing):
        values = [field[c, i] for c in range(6)]
        rate = rates(0, i, values)
        gain, pick = lapse[i], weighted[i]
        for c in range(6):
            value = values[c] + time_step * rate[c]
            section[c, i] = value
            masked[0][c, at(i), :] = value * pick
            keep_product(1, c, i, gain * value)
        return nothing

    def second_step(i, nothing):
        values = [section[c, i] for c in range(6)]
        rate = rates(1, i, values)
        pick = weighted[i]
        for c in range(6):
            value = 0.5 * (field[c, i] + values[c] + time_step * rate[c])
            fresh[c, i] = value
            masked[1][c, at(i), :] = value * pick
        return nothing

    landed(first_pair, 0)
    first_sum[...] = first_part[...] + first_pair[...]
    for d in range(1, half):
        send(first_sum.at[lax.rem(spot + d, half)], first_plane.at[d - 1], in_half(d), 2)
    mat[0:248] = old[0:248]
    mat[248:252] = old[248:252]
    mat[252:256] = jnp.zeros((4, mat.shape[1]), jnp.float32)
    remaining = nt(mat[128:256], mat[...])
    other_part[0] = remaining[:, :128].reshape(tiles)
    other_part[1] = remaining[:, 128:].reshape(tiles)
    send(other_part.at[other], other_pair, {"row": y * 2 + other}, 1)
    for copy in halos[0][4:]:
        copy.wait_recv()
    beyond(0)
    landed(other_pair, 1)
    other_sum[...] = other_part[core] + other_pair[...]
    for d in range(1, half):
        send(other_sum.at[lax.rem(spot + d, half)], other_plane.at[d - 1], in_half(d), 3)
    for copy in halos[0][:4]:
        copy.wait_recv()
    zero_ends(0)
    unrolled(first_step, 0)
    for copy in halos[1][:4]:
        copy.start()
    keep_edges(1)
    for copy in halos[1][4:]:
        copy.start()
    sample(0)

    landed(first_plane, 2)
    total = first_sum[spot]
    for d in range(1, half):
        total = total + first_plane[d - 1]
    first_deep[0] = total
    for d in range(1, n_th):
        send(first_deep.at[0], first_deep.at[d], along(d), 4)
    for copy in halos[1][4:]:
        copy.wait_recv()
    beyond(1)
    landed(other_plane, 3)
    total = other_sum[spot]
    for d in range(1, half):
        total = total + other_plane[d - 1]
    other_deep[0] = total
    for d in range(1, n_th):
        send(other_deep.at[0], other_deep.at[d], along(d), 5)

    for copy in halos[1][:4]:
        copy.wait_recv()
    zero_ends(1)
    unrolled(second_step, 0)
    sample(1)
    landed(first_deep.at[1:], 4)
    total = first_deep[th]
    for a in range(1, n_th):
        total = total + first_deep[lax.rem(th - a + n_th, n_th)]
    first_full[spot] = total
    for d in range(1, half):
        send(first_full.at[spot], first_full.at[spot], in_half(d), 6)
    place_row = lax.broadcasted_iota(jnp.int32, (8, mat.shape[1]), 0)
    snap = jnp.where(place_row >= 4, mat[248:256], 0.0)
    cross_plane[0] = nt(snap, mat[...])[4:8]
    for d in range(1, chunks):
        send(cross_plane.at[0], cross_plane.at[d], in_plane(d), 9)
    stores = [pltpu.make_async_copy(fresh, new_ref, store_sem.at[0])]
    stores[0].start()
    square = lax.broadcasted_iota(jnp.int32, (128, 128), 0)
    column = lax.broadcasted_iota(jnp.int32, (128, 128), 1)
    unit = (square == column).astype(jnp.float32)
    work[:, 128:] = unit
    landed(other_deep.at[1:], 5)
    total = other_deep[th]
    for a in range(1, n_th):
        total = total + other_deep[lax.rem(th - a + n_th, n_th)]
    other_full[owner] = total
    for d in range(1, chunks):
        send(other_full.at[owner], other_full.at[owner], in_plane(d), 7)

    landed(first_plane, 6)
    work[:, :128] = first_full[...].reshape(128, 128)
    def sum_cross():
        landed(cross_plane.at[1:], 9)
        total = cross_plane[owner]
        for a in range(1, chunks):
            total = total + cross_plane[lax.rem(owner - a + chunks, chunks)]
        cross_deep[0] = total
        for d in range(1, n_th):
            send(cross_deep.at[0], cross_deep.at[d], along(d), 10)
        left(first_pair, 0)
        left(other_pair, 1)
        left(first_plane, 2)
        left(other_plane, 3)

    leaf(work, upper, inverse, sum_cross)
    landed(other_full.at[1:], 7)
    first = inverse[...]
    corner = nt(first, other_full[0:half].reshape(128, 128))
    blocks[0] = first
    blocks[1] = upper[...]
    blocks[2] = corner
    last = (square >= 124) | (column >= 124)
    work[:, :128] = jnp.where(last, unit, other_full[half:chunks].reshape(128, 128) - tn(corner, corner))
    work[:, 128:] = unit
    solved_rows = nn(first, mat[0:128])
    rows[0:128] = solved_rows
    rows[128:256] = mat[128:256] - tn(corner, solved_rows)
    blocks[3] = tn(corner, first)

    def hand_over():
        for source, target in ((rows, rows_ref), (blocks.at[0:4], blocks_ref.at[0:4])):
            stores.append(pltpu.make_async_copy(source, target, store_sem.at[len(stores)]))
            stores[-1].start()

    leaf(work, upper, inverse, hand_over)
    blocks[4] = upper[...]
    blocks[5] = inverse[...]
    stores.append(pltpu.make_async_copy(blocks.at[4:6], blocks_ref.at[4:6], store_sem.at[3]))
    stores[-1].start()
    landed(cross_deep.at[1:], 10)
    cross = cross_deep[th]
    for a in range(1, n_th):
        cross = cross + cross_deep[lax.rem(th - a + n_th, n_th)]
    cross_sum[...] = jnp.concatenate([jnp.zeros((4, 256), jnp.float32), cross], axis=0)
    stores.append(pltpu.make_async_copy(cross_sum, cross_ref, store_sem.at[4]))
    stores[-1].start()

    for stage in range(2):
        for copy in halos[stage]:
            copy.wait_send()
    left(first_deep.at[1:], 4)
    left(other_deep.at[1:], 5)
    left(first_plane, 6)
    left(other_full.at[1:], 7)
    left(cross_plane.at[1:], 9)
    left(cross_deep.at[1:], 10)
    for store in stores:
        store.wait()


def finish_kernel(
    scale,
    new_ref, rows_ref, blocks_ref, cross_ref,
    out_new_ref, basis_ref, factor_ref,
    new, rows, blocks, cross_sum, padded_low, basis, factor,
    load_sem, store_sem,
):
    loads = (
        (blocks_ref, blocks), (cross_ref, cross_sum), (rows_ref.at[128:256], rows.at[128:256]),
        (rows_ref.at[0:128], rows.at[0:128]), (new_ref, new),
    )
    loads = [pltpu.make_async_copy(source, target, load_sem.at[k]) for k, (source, target) in enumerate(loads)]
    for load in loads:
        load.start()
    factor[128:256, 0:128] = jnp.zeros((128, 128), jnp.float32)
    padded_low[...] = jnp.zeros_like(padded_low)
    for load in loads[:4]:
        load.wait()
    first, second, corner = blocks[0], blocks[5], blocks[2]
    factor[0:128, 0:128] = blocks[1] * (1.0 / scale)
    basis[0:128] = rows[0:128] * scale
    below = -nn(second, blocks[3])
    cross = cross_sum[...]
    cross_left, cross_right = cross[:, :128], cross[:, 128:]
    lane8 = lax.broadcasted_iota(jnp.int32, (8, 128), 1)
    sub8 = lax.broadcasted_iota(jnp.int32, (8, 128), 0)
    inner = jnp.where(lane8 < 124, cross_right, 0.0)
    low_left = nt(cross_left, first)
    low_right = jnp.where(lane8 < 124, nt(cross_left, below) + nt(inner, second), 0.0)
    padded_low[120:128, 0:128] = low_left
    padded_low[120:128, 128:256] = low_right
    low = jnp.concatenate([low_left, low_right], axis=1)
    place_row = lax.broadcasted_iota(jnp.int32, (8, basis.shape[1]), 0)
    snap = jnp.where(place_row >= 4, rows[248:256], 0.0)
    basis[128:256] = nn(second, rows[128:256]) * scale
    stores = [
        pltpu.make_async_copy(source, target, store_sem.at[k])
        for k, (source, target) in enumerate(
            (
                (new, out_new_ref),
                (basis.at[0:128], basis_ref.at[0:128]),
                (basis.at[128:256], basis_ref.at[128:256]),
                (factor, factor_ref),
            )
        )
    ]
    loads[4].wait()
    for store in stores[:2]:
        store.start()
    snapshot_block = cross_right - nt(low, padded_low[...])
    real = sub8 >= 4
    diagonal = (lane8 == sub8 + 120).astype(jnp.float32)
    snapshot_block = jnp.where(real & (lane8 >= 124), snapshot_block, diagonal)
    rest = snap * scale - nn(low, basis[...])
    _, _, _, solved = eliminate(spread(snapshot_block, 120), jnp.concatenate([snapshot_block, rest], axis=1))
    basis[248:256] = jnp.where(place_row >= 4, solved[:, 128:], basis[248:256])
    turned = padded_low[...].T
    square = lax.broadcasted_iota(jnp.int32, (128, 128), 0)
    column = lax.broadcasted_iota(jnp.int32, (128, 128), 1)
    factor[0:128, 128:256] = jnp.where(column >= 124, turned[0:128], corner) * (1.0 / scale)
    factor[128:256, 128:256] = jnp.where(column >= 124, turned[128:256], blocks[4]) * (1.0 / scale)
    finish = jnp.where(lane8 >= sub8 + 120, solved[:, :128] * (1.0 / scale), 0.0)
    factor[248:256, 128:256] = jnp.where(real, finish, factor[248:256, 128:256])
    for store in stores[2:]:
        store.start()
    for store in stores:
        store.wait()


def on_device(sizes, fields, lapse_field, excision, sample_cells, old_basis):
    n_row, n_th, n_ph = sizes
    cr, ct, cp = lapse_field.shape
    columns = old_basis.shape[1]
    f32 = jnp.float32
    half = n_row * n_ph // 2
    rows = 128 // half
    cells = sample_cells.reshape(cr, ct)
    vmem = pltpu.VMEM
    scale = math.sqrt(columns * n_row * n_th * n_ph)
    between = (
        jax.ShapeDtypeStruct(fields.shape, f32),
        jax.ShapeDtypeStruct((256, columns), f32),
        jax.ShapeDtypeStruct((6, 128, 128), f32),
        jax.ShapeDtypeStruct((8, 256), f32),
    )
    outputs = (
        jax.ShapeDtypeStruct(fields.shape, f32),
        jax.ShapeDtypeStruct((256, columns), f32),
        jax.ShapeDtypeStruct((256, 256), f32),
    )
    results = pl.pallas_call(
        functools.partial(comm_kernel, sizes, scale),
        out_shape=between,
        in_specs=[HBM] * 5,
        out_specs=(HBM,) * 4,
        scratch_shapes=[
            vmem(fields.shape, f32),
            vmem(lapse_field.shape, f32),
            vmem(excision.shape, jnp.int32),
            vmem(cells.shape, jnp.int32),
            vmem(old_basis.shape, f32),
            vmem((256, columns), f32),
            vmem(fields.shape, f32),
            vmem(fields.shape, f32),
            vmem(lapse_field.shape, f32),
            vmem((6, cr * ct, cp), f32),
            vmem((6, cr * ct, cp), f32),
            vmem((6, cr + 4, 32, cp), f32),
            vmem((6, cr + 4, 32, cp), f32),
            vmem((2, 4, 2, cr, cp), f32),
            vmem((2, 4, 2, cr, cp), f32),
            vmem((2, 4, 2, cr, cp), f32),
            vmem((2, 4, 2, cr, cp), f32),
            vmem((2, ct, cp), f32),
            vmem((2, ct, cp), f32),
            vmem((2, ct, cp), f32),
            vmem((2, ct, cp), f32),
            vmem((4, cr, ct, cp), f32),
            vmem((half, rows, 128), f32),
            vmem((half, rows, 128), f32),
            vmem((half, rows, 128), f32),
            vmem((half - 1, rows, 128), f32),
            vmem((n_th, rows, 128), f32),
            vmem((half, rows, 128), f32),
            vmem((2, half, rows, 128), f32),
            vmem((half, rows, 128), f32),
            vmem((half, rows, 128), f32),
            vmem((half - 1, rows, 128), f32),
            vmem((n_th, rows, 128), f32),
            vmem((2 * half, rows, 128), f32),
            vmem((2 * half, 4, 256), f32),
            vmem((n_th, 4, 256), f32),
            vmem((128, 256), f32),
            vmem((128, 128), f32),
            vmem((128, 128), f32),
            vmem((256, columns), f32),
            vmem((6, 128, 128), f32),
            vmem((8, 256), f32),
            pltpu.SemaphoreType.DMA((6,)),
            pltpu.SemaphoreType.DMA((5,)),
            pltpu.SemaphoreType.DMA((2, 6)),
            pltpu.SemaphoreType.DMA((2, 6)),
            pltpu.SemaphoreType.DMA((11,)),
            pltpu.SemaphoreType.DMA((11,)),
        ],
        compiler_params=pltpu.CompilerParams(
            collective_id=0, has_side_effects=True, vmem_limit_bytes=LIMIT
        ),
        name="halo_and_gram",
    )(fields, lapse_field, excision, cells, old_basis)
    return pl.pallas_call(
        functools.partial(finish_kernel, scale),
        out_shape=outputs,
        in_specs=[HBM] * 4,
        out_specs=(HBM,) * 3,
        scratch_shapes=[vmem(array.shape, f32) for array in between]
        + [vmem((128, 256), f32), vmem((256, columns), f32), vmem((256, 256), f32)]
        + [pltpu.SemaphoreType.DMA((5,)), pltpu.SemaphoreType.DMA((4,))],
        compiler_params=pltpu.CompilerParams(vmem_limit_bytes=LIMIT),
        name="finish",
    )(*results)


def solution(mesh):
    sizes = tuple(mesh.shape[name] for name in ("row", "th", "ph"))
    return jax.shard_map(
        functools.partial(on_device, sizes),
        mesh=mesh,
        in_specs=(
            P(None, "row", "th", "ph"),
            P("row", "th", "ph"),
            P("row", "th", "ph"),
            P("row", "th", "ph"),
            P(None, ("row", "th", "ph")),
        ),
        out_specs=(P(None, "row", "th", "ph"), P(None, ("row", "th", "ph")), P()),
        check_vma=False,
    )
```

```python
import functools
import math

import jax
import jax.numpy as jnp
from jax import lax
from jax.experimental import pallas as pl
from jax.experimental.pallas import tpu as pltpu
from jax.sharding import PartitionSpec as P

MESH = pl.DeviceIdType.MESH
LIMIT = 63 * 1024 * 1024
UNROLL = 4
MIDWAY = 10
HIGH = lax.Precision.HIGHEST
HBM = pl.BlockSpec(memory_space=pltpu.HBM)

damping_rate = 3.0
time_step = 0.3
azimuth_gain = 5.0

SLOT = {0: 0, 3: 1, 2: 2, 5: 3, 1: 4, 4: 5}
EDGE = {0: 0, 3: 1, 1: 2, 4: 3}


def nt(a, b):
    return lax.dot_general(a, b, (((1,), (1,)), ((), ())), precision=HIGH, preferred_element_type=jnp.float32)


def nn(a, b):
    return lax.dot_general(a, b, (((1,), (0,)), ((), ())), precision=HIGH, preferred_element_type=jnp.float32)


def tn(a, b):
    return lax.dot_general(a, b, (((0,), (0,)), ((), ())), precision=HIGH, preferred_element_type=jnp.float32)


def diff(near_high, near_low, far_high, far_low, gain):
    return (8.0 * (near_high - near_low) - (far_high - far_low)) * (gain / 12.0)


def sublane(x, k):
    return jnp.broadcast_to(x[k : k + 1], x.shape)


def eliminate(columns, x, follower=None):
    sub = lax.broadcasted_iota(jnp.int32, x.shape, 0)
    columns = list(columns)
    lows, recips, rows = [], [], []
    solved = jnp.zeros_like(x)
    for k in range(8):
        recip = lax.rsqrt(sublane(columns[k], k))
        low = columns[k] * recip
        for b in range(k + 1, 8):
            columns[b] = columns[b] - low * sublane(low, b)
        wide = jnp.tile(recip, (1, x.shape[1] // 128))
        line = sublane(x, k) * wide
        x = x - jnp.tile(low, (1, x.shape[1] // 128)) * line
        solved = jnp.where(sub == k, line, solved)
        lows.append(low)
        recips.append(recip)
        rows.append(line)
        if follower is not None:
            follower(k, recip, low, line)
    return lows, recips, rows, solved


def spread(tile, first):
    return [jnp.broadcast_to(tile[:, first + b : first + b + 1], (8, 128)) for b in range(8)]


def twice(x):
    return jnp.concatenate([x, x], axis=1)


def leaf(work, upper, inverse, midway=None):
    lane = lax.broadcasted_iota(jnp.int32, (8, 128), 1)
    sub = lax.broadcasted_iota(jnp.int32, (8, 128), 0)
    tiles = {t: work[8 * t : 8 * t + 8] for t in range(2)}
    columns = spread(tiles[0], 0)
    for p in range(16):
        if p == MIDWAY and midway is not None:
            midway()
        r0 = 8 * p
        if p < 14:
            tiles[p + 2] = work[r0 + 16 : r0 + 24]
        near = spread(tiles[p + 1], r0) if p < 15 else None
        ahead = spread(tiles[p + 1], r0 + 8) if p < 15 else None
        far = spread(tiles[p + 2], r0) if p < 14 else None

        def follower(k, recip, low, line):
            for t, column in ((p + 1, near), (p + 2, far)):
                if column is None:
                    continue
                mine = column[k] * recip
                tiles[t] = tiles[t] - twice(mine) * line
                for b in range(k + 1, 8):
                    column[b] = column[b] - mine * sublane(low, b)
                if t == p + 1:
                    for b in range(8):
                        ahead[b] = ahead[b] - mine * sublane(mine, b)

        lows, recips, rows, solved = eliminate(columns, tiles[p], follower)
        upper[r0 : r0 + 8] = jnp.where(lane >= sub + r0, solved[:, :128], 0.0)
        inverse[r0 : r0 + 8] = solved[:, 128:]
        columns = ahead
        if p < 13:
            back = [None] * 8
            for q in range(7, -1, -1):
                value = rows[q]
                for a in range(q + 1, 8):
                    value = value - twice(sublane(lows[q], a)) * back[a]
                back[q] = value * twice(recips[q])
            for t in range(p + 3, 16):
                tile = work[8 * t : 8 * t + 8]
                for k, column in enumerate(spread(tile, r0)):
                    tile = tile - twice(column) * back[k]
                work[8 * t : 8 * t + 8] = tile


def comm_kernel(
    sizes, scale,
    fields_ref, lapse_ref, excision_ref, cells_ref, old_ref,
    new_ref, rows_ref, blocks_ref, cross_ref,
    field, lapse, excision, cells, old, mat, fresh, section, weighted, masked0, masked1,
    padded0, padded1, polar_out0, polar_out1, polar_in0, polar_in1, edge_out0, edge_out1, edge_in0, edge_in1, outside,
    first_part, first_pair, first_sum, first_plane, first_deep, first_full,
    other_part, other_pair, other_sum, other_plane, other_deep, other_full,
    cross_plane, cross_deep,
    work, upper, inverse, rows, blocks, cross_sum,
    load_sem, store_sem, halo_send, halo_recv, send_sem, recv_sem,
):
    masked, padded = (masked0, masked1), (padded0, padded1)
    polar_out, polar_in = (polar_out0, polar_out1), (polar_in0, polar_in1)
    edge_out, edge_in = (edge_out0, edge_out1), (edge_in0, edge_in1)
    n_row, n_th, n_ph = sizes
    n_y = n_row // 2
    row, th, ph = lax.axis_index("row"), lax.axis_index("th"), lax.axis_index("ph")
    core, y = lax.rem(row, 2), lax.div(row, 2)
    spot = y * n_ph + ph
    half = n_y * n_ph
    chunks = 2 * half
    owner = core * half + spot
    cr, ct, cp = 16, 16, 128

    loads = [
        pltpu.make_async_copy(source, target, load_sem.at[k])
        for k, (source, target) in enumerate(
            (
                (old_ref.at[0:128], old.at[0:128]),
                (fields_ref, field),
                (lapse_ref, lapse),
                (excision_ref, excision),
                (cells_ref, cells),
                (old_ref.at[128:252], old.at[128:252]),
            )
        )
    ]
    for load in loads:
        load.start()

    def place(index):
        which, rest = lax.div(index, half), lax.rem(index, half)
        return {"row": lax.div(rest, n_ph) * 2 + which, "ph": lax.rem(rest, n_ph)}

    def in_plane(d):
        return place(lax.rem(owner + d, chunks))

    def in_half(d):
        return place(core * half + lax.rem(spot + d, half))

    def along(d):
        return {"th": lax.rem(th + d, n_th)}

    barrier = pltpu.get_barrier_semaphore()
    for d in range(1, chunks):
        pl.semaphore_signal(barrier, inc=1, device_id=in_plane(d), device_id_type=MESH)
    for d in range(1, n_th):
        pl.semaphore_signal(barrier, inc=1, device_id=along(d), device_id_type=MESH)

    def send(source, target, device, k):
        copy = pltpu.make_async_remote_copy(
            src_ref=source, dst_ref=target, send_sem=send_sem.at[k], recv_sem=recv_sem.at[k],
            device_id=device, device_id_type=MESH,
        )
        copy.start()

    def landed(ref, k):
        pltpu.make_async_copy(ref, ref, recv_sem.at[k]).wait()

    def left(ref, k):
        pltpu.make_async_copy(ref, ref, send_sem.at[k]).wait()

    lane = lax.broadcasted_iota(jnp.int32, (ct, cp), 1)
    lane_pair = lax.shift_right_logical(lane, 1)

    loads[0].wait()
    tiles = first_part.shape
    first_part[...] = nt(old[0:128], old[0:128]).reshape(tiles)
    pl.semaphore_wait(barrier, chunks - 1 + n_th - 1)
    other = 1 - core
    send(first_part, first_pair, {"row": y * 2 + other}, 0)

    def keep_product(stage, c, i, value):
        slot = SLOT[c]
        padded[stage][slot, i + 2, 8:24, :] = value
        if slot < 4:
            for s in range(2):
                polar_out[stage][0, slot, s, pl.ds(i, 1), :] = value[s : s + 1]
                polar_out[stage][1, slot, s, pl.ds(i, 1), :] = value[14 + s : 15 + s]

    def keep_edges(stage):
        low = high = jnp.zeros((ct, cp), jnp.float32)
        for c, e in EDGE.items():
            for i in range(cr):
                t = e * cr + i
                value = padded[stage][SLOT[c], i + 2, 8:24, :]
                here = lane_pair == t
                low = jnp.where(here, pltpu.roll(value, 2 * t, 1), low)
                high = jnp.where(here, pltpu.roll(value, (2 * t + 2) % cp, 1), high)
        edge_out[stage][0] = low
        edge_out[stage][1] = high

    def beyond(stage):
        low, high = edge_in[stage][0], edge_in[stage][1]
        for e in range(4):
            for i in range(cr):
                t = e * cr + i
                moved = pltpu.roll(high, (cp - 2 * t) % cp, 1), pltpu.roll(low, cp - 2 - 2 * t, 1)
                outside[e, i] = jnp.where(lane < cp // 2, *moved)

    def unrolled(body, carry, by=UNROLL):
        def several(k, carry):
            for u in range(by):
                carry = body(k * by + u, carry)
            return carry

        if by == cr:
            return several(0, carry)
        return lax.fori_loop(0, cr // by, several, carry)

    def sample(stage):
        for c in range(6):
            for h in range(cr * ct // cp):
                line = jnp.sum(masked[stage][c, h * cp : (h + 1) * cp, :].T, axis=0, keepdims=True)
                r, first = 252 + 2 * stage + c // 3, (c % 3) * cr * ct + h * cp
                mat[r : r + 1, first : first + cp] = line

    def at(i):
        return slice(i * ct, (i + 1) * ct) if isinstance(i, int) else pl.ds(pl.multiple_of(i * ct, ct), ct)

    def first_products(i, nothing):
        gain = lapse[i]
        for c in range(6):
            keep_product(0, c, i, gain * field[c, i])
        return nothing

    def halo_copies(stage):
        rows = ((padded[stage].at[2:6, 2:4, 8:24, :], padded[stage].at[2:6, 18:20, 8:24, :], {"row": lax.rem(row + n_row - 1, n_row)}),
                (padded[stage].at[2:6, 16:18, 8:24, :], padded[stage].at[2:6, 0:2, 8:24, :], {"row": lax.rem(row + 1, n_row)}))
        polars = ((polar_out[stage].at[0], polar_in[stage].at[1], {"th": lax.rem(th + n_th - 1, n_th)}),
                  (polar_out[stage].at[1], polar_in[stage].at[0], {"th": lax.rem(th + 1, n_th)}))
        edges = ((edge_out[stage].at[0], edge_in[stage].at[1], {"ph": lax.rem(ph + n_ph - 1, n_ph)}),
                 (edge_out[stage].at[1], edge_in[stage].at[0], {"ph": lax.rem(ph + 1, n_ph)}))
        return [
            pltpu.make_async_remote_copy(
                src_ref=source, dst_ref=target, send_sem=halo_send.at[stage, k], recv_sem=halo_recv.at[stage, k],
                device_id=device, device_id_type=MESH,
            )
            for k, (source, target, device) in enumerate(rows + polars + edges)
        ]

    for load in loads[1:]:
        load.wait()
    unrolled(first_products, 0, cr)
    keep_edges(0)

    halos = [halo_copies(0), halo_copies(1)]
    for copy in halos[0]:
        copy.start()
    pol_index = (th * ct + lax.broadcasted_iota(jnp.int32, (ct, cp), 0)).astype(jnp.float32)
    polar = jnp.pi * (pol_index + 0.5) / (n_th * ct)
    polar_weight = jnp.sqrt(jnp.sin(polar))
    chosen = cells[...].T
    for i in range(cr):
        radius = 1.0 + 2.0 * ((row * cr + i).astype(jnp.float32) + 0.5) / (n_row * cr)
        weighted[i] = jnp.where(lane == chosen[:, i : i + 1], polar_weight * radius, 0.0)

    def rates(stage, i, c_values):
        damped = damping_rate * excision[i].astype(jnp.float32)
        for slot in range(4):
            for s in range(2):
                low = polar_in[stage][0, slot, s, pl.ds(i, 1), :]
                high = polar_in[stage][1, slot, s, pl.ds(i, 1), :]
                padded[stage][slot, i + 2, 6 + s : 7 + s, :] = jnp.where(th > 0, low, 0.0)
                padded[stage][slot, i + 2, 24 + s : 25 + s, :] = jnp.where(th < n_th - 1, high, 0.0)

        def rad(c):
            get = lambda o: padded[stage][SLOT[c], i + 2 + o, 8:24, :]
            return diff(get(1), get(-1), get(2), get(-2), 1.0)

        def pol(c):
            get = lambda o: padded[stage][SLOT[c], i + 2, 8 + o : 24 + o, :]
            return diff(get(1), get(-1), get(2), get(-2), 1.0)

        def azi(c):
            here = padded[stage][SLOT[c], i + 2, 8:24, :]
            edge = outside[EDGE[c], i]
            far_low = pltpu.roll(jnp.where(lane >= cp - 2, edge, here), 2, 1)
            near_low = pltpu.roll(jnp.where(lane >= cp - 1, edge, here), 1, 1)
            near_high = pltpu.roll(jnp.where(lane < 1, edge, here), cp - 1, 1)
            far_high = pltpu.roll(jnp.where(lane < 2, edge, here), cp - 2, 1)
            return diff(near_high, near_low, far_high, far_low, azimuth_gain)

        out = []
        for start, sign in ((3, 1.0), (0, -1.0)):
            curls = (pol(start + 2) - azi(start + 1), azi(start) - rad(start + 2), rad(start + 1) - pol(start))
            for k in range(3):
                c = len(out)
                out.append((curls[k] if sign > 0 else -curls[k]) - damped * c_values[c])
        return out

    def zero_ends(stage):
        low = padded[stage][2:6, 0:2, 8:24, :]
        padded[stage][2:6, 0:2, 8:24, :] = jnp.where(row > 0, low, 0.0)
        high = padded[stage][2:6, 18:20, 8:24, :]
        padded[stage][2:6, 18:20, 8:24, :] = jnp.where(row < n_row - 1, high, 0.0)

    def first_step(i, nothing):
        values = [field[c, i] for c in range(6)]
        rate = rates(0, i, values)
        gain, pick = lapse[i], weighted[i]
        for c in range(6):
            value = values[c] + time_step * rate[c]
            section[c, i] = value
            masked[0][c, at(i), :] = value * pick
            keep_product(1, c, i, gain * value)
        return nothing

    def second_step(i, nothing):
        values = [section[c, i] for c in range(6)]
        rate = rates(1, i, values)
        pick = weighted[i]
        for c in range(6):
            value = 0.5 * (field[c, i] + values[c] + time_step * rate[c])
            fresh[c, i] = value
            masked[1][c, at(i), :] = value * pick
        return nothing

    landed(first_pair, 0)
    first_sum[...] = first_part[...] + first_pair[...]
    for d in range(1, half):
        send(first_sum.at[lax.rem(spot + d, half)], first_plane.at[d - 1], in_half(d), 2)
    mat[0:248] = old[0:248]
    mat[248:252] = old[248:252]
    mat[252:256] = jnp.zeros((4, mat.shape[1]), jnp.float32)
    remaining = nt(mat[128:256], mat[...])
    other_part[0] = remaining[:, :128].reshape(tiles)
    other_part[1] = remaining[:, 128:].reshape(tiles)
    send(other_part.at[other], other_pair, {"row": y * 2 + other}, 1)
    for copy in halos[0][4:]:
        copy.wait_recv()
    beyond(0)
    landed(other_pair, 1)
    other_sum[...] = other_part[core] + other_pair[...]
    for d in range(1, half):
        send(other_sum.at[lax.rem(spot + d, half)], other_plane.at[d - 1], in_half(d), 3)
    for copy in halos[0][:4]:
        copy.wait_recv()
    zero_ends(0)
    unrolled(first_step, 0)
    for copy in halos[1][:4]:
        copy.start()
    keep_edges(1)
    for copy in halos[1][4:]:
        copy.start()
    sample(0)

    landed(first_plane, 2)
    total = first_sum[spot]
    for d in range(1, half):
        total = total + first_plane[d - 1]
    first_deep[0] = total
    for d in range(1, n_th):
        send(first_deep.at[0], first_deep.at[d], along(d), 4)
    landed(other_plane, 3)
    total = other_sum[spot]
    for d in range(1, half):
        total = total + other_plane[d - 1]
    other_deep[0] = total
    for d in range(1, n_th):
        send(other_deep.at[0], other_deep.at[d], along(d), 5)

    for copy in halos[1][4:]:
        copy.wait_recv()
    beyond(1)
    for copy in halos[1][:4]:
        copy.wait_recv()
    zero_ends(1)
    unrolled(second_step, 0)
    sample(1)
    landed(first_deep.at[1:], 4)
    total = first_deep[th]
    for a in range(1, n_th):
        total = total + first_deep[lax.rem(th - a + n_th, n_th)]
    first_full[spot] = total
    for d in range(1, half):
        send(first_full.at[spot], first_full.at[spot], in_half(d), 6)
    place_row = lax.broadcasted_iota(jnp.int32, (8, mat.shape[1]), 0)
    snap = jnp.where(place_row >= 4, mat[248:256], 0.0)
    cross_plane[0] = nt(snap, mat[...])[4:8]
    for d in range(1, chunks):
        send(cross_plane.at[0], cross_plane.at[d], in_plane(d), 9)
    stores = [pltpu.make_async_copy(fresh, new_ref, store_sem.at[0])]
    stores[0].start()
    square = lax.broadcasted_iota(jnp.int32, (128, 128), 0)
    column = lax.broadcasted_iota(jnp.int32, (128, 128), 1)
    unit = (square == column).astype(jnp.float32)
    work[:, 128:] = unit
    landed(other_deep.at[1:], 5)
    total = other_deep[th]
    for a in range(1, n_th):
        total = total + other_deep[lax.rem(th - a + n_th, n_th)]
    other_full[owner] = total
    for d in range(1, chunks):
        send(other_full.at[owner], other_full.at[owner], in_plane(d), 7)

    landed(first_plane, 6)
    work[:, :128] = first_full[...].reshape(128, 128)
    def sum_cross():
        landed(cross_plane.at[1:], 9)
        total = cross_plane[owner]
        for a in range(1, chunks):
            total = total + cross_plane[lax.rem(owner - a + chunks, chunks)]
        cross_deep[0] = total
        for d in range(1, n_th):
            send(cross_deep.at[0], cross_deep.at[d], along(d), 10)
        left(first_pair, 0)
        left(other_pair, 1)
        left(first_plane, 2)
        left(other_plane, 3)

    leaf(work, upper, inverse, sum_cross)
    landed(other_full.at[1:], 7)
    first = inverse[...]
    corner = nt(first, other_full[0:half].reshape(128, 128))
    blocks[0] = first
    blocks[1] = upper[...]
    blocks[2] = corner
    last = (square >= 124) | (column >= 124)
    work[:, :128] = jnp.where(last, unit, other_full[half:chunks].reshape(128, 128) - tn(corner, corner))
    work[:, 128:] = unit
    solved_rows = nn(first, mat[0:128])
    rows[0:128] = solved_rows
    rows[128:256] = mat[128:256] - tn(corner, solved_rows)
    blocks[3] = tn(corner, first)

    def hand_over():
        for source, target in ((rows, rows_ref), (blocks.at[0:4], blocks_ref.at[0:4])):
            stores.append(pltpu.make_async_copy(source, target, store_sem.at[len(stores)]))
            stores[-1].start()

    leaf(work, upper, inverse, hand_over)
    blocks[4] = upper[...]
    blocks[5] = inverse[...]
    stores.append(pltpu.make_async_copy(blocks.at[4:6], blocks_ref.at[4:6], store_sem.at[3]))
    stores[-1].start()
    landed(cross_deep.at[1:], 10)
    cross = cross_deep[th]
    for a in range(1, n_th):
        cross = cross + cross_deep[lax.rem(th - a + n_th, n_th)]
    cross_sum[...] = jnp.concatenate([jnp.zeros((4, 256), jnp.float32), cross], axis=0)
    stores.append(pltpu.make_async_copy(cross_sum, cross_ref, store_sem.at[4]))
    stores[-1].start()

    for stage in range(2):
        for copy in halos[stage]:
            copy.wait_send()
    left(first_deep.at[1:], 4)
    left(other_deep.at[1:], 5)
    left(first_plane, 6)
    left(other_full.at[1:], 7)
    left(cross_plane.at[1:], 9)
    left(cross_deep.at[1:], 10)
    for store in stores:
        store.wait()


def finish_kernel(
    scale,
    new_ref, rows_ref, blocks_ref, cross_ref,
    out_new_ref, basis_ref, factor_ref,
    new, rows, blocks, cross_sum, padded_low, basis, factor,
    load_sem, store_sem,
):
    loads = (
        (blocks_ref, blocks), (cross_ref, cross_sum), (rows_ref.at[128:256], rows.at[128:256]),
        (rows_ref.at[0:128], rows.at[0:128]), (new_ref, new),
    )
    loads = [pltpu.make_async_copy(source, target, load_sem.at[k]) for k, (source, target) in enumerate(loads)]
    for load in loads:
        load.start()
    factor[128:256, 0:128] = jnp.zeros((128, 128), jnp.float32)
    padded_low[...] = jnp.zeros_like(padded_low)
    for load in loads[:4]:
        load.wait()
    first, second, corner = blocks[0], blocks[5], blocks[2]
    factor[0:128, 0:128] = blocks[1] * (1.0 / scale)
    basis[0:128] = rows[0:128] * scale
    below = -nn(second, blocks[3])
    cross = cross_sum[...]
    cross_left, cross_right = cross[:, :128], cross[:, 128:]
    lane8 = lax.broadcasted_iota(jnp.int32, (8, 128), 1)
    sub8 = lax.broadcasted_iota(jnp.int32, (8, 128), 0)
    inner = jnp.where(lane8 < 124, cross_right, 0.0)
    low_left = nt(cross_left, first)
    low_right = jnp.where(lane8 < 124, nt(cross_left, below) + nt(inner, second), 0.0)
    padded_low[120:128, 0:128] = low_left
    padded_low[120:128, 128:256] = low_right
    low = jnp.concatenate([low_left, low_right], axis=1)
    place_row = lax.broadcasted_iota(jnp.int32, (8, basis.shape[1]), 0)
    snap = jnp.where(place_row >= 4, rows[248:256], 0.0)
    basis[128:256] = nn(second, rows[128:256]) * scale
    stores = [
        pltpu.make_async_copy(source, target, store_sem.at[k])
        for k, (source, target) in enumerate(
            (
                (new, out_new_ref),
                (basis.at[0:128], basis_ref.at[0:128]),
                (basis.at[128:256], basis_ref.at[128:256]),
                (factor, factor_ref),
            )
        )
    ]
    loads[4].wait()
    for store in stores[:2]:
        store.start()
    snapshot_block = cross_right - nt(low, padded_low[...])
    real = sub8 >= 4
    diagonal = (lane8 == sub8 + 120).astype(jnp.float32)
    snapshot_block = jnp.where(real & (lane8 >= 124), snapshot_block, diagonal)
    rest = snap * scale - nn(low, basis[...])
    _, _, _, solved = eliminate(spread(snapshot_block, 120), jnp.concatenate([snapshot_block, rest], axis=1))
    basis[248:256] = jnp.where(place_row >= 4, solved[:, 128:], basis[248:256])
    turned = padded_low[...].T
    square = lax.broadcasted_iota(jnp.int32, (128, 128), 0)
    column = lax.broadcasted_iota(jnp.int32, (128, 128), 1)
    factor[0:128, 128:256] = jnp.where(column >= 124, turned[0:128], corner) * (1.0 / scale)
    factor[128:256, 128:256] = jnp.where(column >= 124, turned[128:256], blocks[4]) * (1.0 / scale)
    finish = jnp.where(lane8 >= sub8 + 120, solved[:, :128] * (1.0 / scale), 0.0)
    factor[248:256, 128:256] = jnp.where(real, finish, factor[248:256, 128:256])
    for store in stores[2:]:
        store.start()
    for store in stores:
        store.wait()


def on_device(sizes, fields, lapse_field, excision, sample_cells, old_basis):
    n_row, n_th, n_ph = sizes
    cr, ct, cp = lapse_field.shape
    columns = old_basis.shape[1]
    f32 = jnp.float32
    half = n_row * n_ph // 2
    rows = 128 // half
    cells = sample_cells.reshape(cr, ct)
    vmem = pltpu.VMEM
    scale = math.sqrt(columns * n_row * n_th * n_ph)
    between = (
        jax.ShapeDtypeStruct(fields.shape, f32),
        jax.ShapeDtypeStruct((256, columns), f32),
        jax.ShapeDtypeStruct((6, 128, 128), f32),
        jax.ShapeDtypeStruct((8, 256), f32),
    )
    outputs = (
        jax.ShapeDtypeStruct(fields.shape, f32),
        jax.ShapeDtypeStruct((256, columns), f32),
        jax.ShapeDtypeStruct((256, 256), f32),
    )
    results = pl.pallas_call(
        functools.partial(comm_kernel, sizes, scale),
        out_shape=between,
        in_specs=[HBM] * 5,
        out_specs=(HBM,) * 4,
        scratch_shapes=[
            vmem(fields.shape, f32),
            vmem(lapse_field.shape, f32),
            vmem(excision.shape, jnp.int32),
            vmem(cells.shape, jnp.int32),
            vmem(old_basis.shape, f32),
            vmem((256, columns), f32),
            vmem(fields.shape, f32),
            vmem(fields.shape, f32),
            vmem(lapse_field.shape, f32),
            vmem((6, cr * ct, cp), f32),
            vmem((6, cr * ct, cp), f32),
            vmem((6, cr + 4, 32, cp), f32),
            vmem((6, cr + 4, 32, cp), f32),
            vmem((2, 4, 2, cr, cp), f32),
            vmem((2, 4, 2, cr, cp), f32),
            vmem((2, 4, 2, cr, cp), f32),
            vmem((2, 4, 2, cr, cp), f32),
            vmem((2, ct, cp), f32),
            vmem((2, ct, cp), f32),
            vmem((2, ct, cp), f32),
            vmem((2, ct, cp), f32),
            vmem((4, cr, ct, cp), f32),
            vmem((half, rows, 128), f32),
            vmem((half, rows, 128), f32),
            vmem((half, rows, 128), f32),
            vmem((half - 1, rows, 128), f32),
            vmem((n_th, rows, 128), f32),
            vmem((half, rows, 128), f32),
            vmem((2, half, rows, 128), f32),
            vmem((half, rows, 128), f32),
            vmem((half, rows, 128), f32),
            vmem((half - 1, rows, 128), f32),
            vmem((n_th, rows, 128), f32),
            vmem((2 * half, rows, 128), f32),
            vmem((2 * half, 4, 256), f32),
            vmem((n_th, 4, 256), f32),
            vmem((128, 256), f32),
            vmem((128, 128), f32),
            vmem((128, 128), f32),
            vmem((256, columns), f32),
            vmem((6, 128, 128), f32),
            vmem((8, 256), f32),
            pltpu.SemaphoreType.DMA((6,)),
            pltpu.SemaphoreType.DMA((5,)),
            pltpu.SemaphoreType.DMA((2, 6)),
            pltpu.SemaphoreType.DMA((2, 6)),
            pltpu.SemaphoreType.DMA((11,)),
            pltpu.SemaphoreType.DMA((11,)),
        ],
        compiler_params=pltpu.CompilerParams(
            collective_id=0, has_side_effects=True, vmem_limit_bytes=LIMIT
        ),
        name="halo_and_gram",
    )(fields, lapse_field, excision, cells, old_basis)
    return pl.pallas_call(
        functools.partial(finish_kernel, scale),
        out_shape=outputs,
        in_specs=[HBM] * 4,
        out_specs=(HBM,) * 3,
        scratch_shapes=[vmem(array.shape, f32) for array in between]
        + [vmem((128, 256), f32), vmem((256, columns), f32), vmem((256, 256), f32)]
        + [pltpu.SemaphoreType.DMA((5,)), pltpu.SemaphoreType.DMA((4,))],
        compiler_params=pltpu.CompilerParams(vmem_limit_bytes=LIMIT),
        name="finish",
    )(*results)


def solution(mesh):
    sizes = tuple(mesh.shape[name] for name in ("row", "th", "ph"))
    return jax.shard_map(
        functools.partial(on_device, sizes),
        mesh=mesh,
        in_specs=(
            P(None, "row", "th", "ph"),
            P("row", "th", "ph"),
            P("row", "th", "ph"),
            P("row", "th", "ph"),
            P(None, ("row", "th", "ph")),
        ),
        out_specs=(P(None, "row", "th", "ph"), P(None, ("row", "th", "ph")), P()),
        check_vma=False,
    )
```
